32 devices in a mesh: dp: 2 (over x), ctx: 2 (over y), expert: 8 (over z, core).
Axes of the slice: x: 2, y: 2, z: 4, core: 2. Of those that a mesh axis runs over, the one named last changes fastest.
Arguments:
- layer_input: bfloat16 [16, 256, 2048], P(('dp', 'expert'), 'ctx'), may hold values from -6 to 6
- cotangent: bfloat16 [16, 256, 2048], P(('dp', 'expert'), 'ctx'), may hold values from -6 to 6
- routes: int32 [16, 256, 6], P(('dp', 'expert'), 'ctx'), may hold values from 0 to 15, all different within a row; in each aligned block of 128 rows (0 to 127, 128 to 255, ..., all dimensions but the last counted through in order) at most 64 rows name the same one
- attn_gain: float32 [2048], replicated, may hold values from 0.5 to 1.5
- w_query: bfloat16 [2048, 3072], P('expert'), may hold values from -0.125 to 0.125
- w_latent: bfloat16 [2048, 576], P('expert'), may hold values from -0.125 to 0.125
- latent_gain: float32 [512], replicated, may hold values from 0.5 to 1.5
- w_expand: bfloat16 [512, 4096], P('expert'), may hold values from -0.25 to 0.25
- w_output: bfloat16 [2048, 2048], P('expert'), may hold values from -0.5 to 0.5
- ffn_gain: float32 [2048], replicated, may hold values from 0.5 to 1.5
- w_router: bfloat16 [2048, 16], P('expert'), may hold values from -0.125 to 0.125
- w_shared_in: bfloat16 [2048, 5632], P('expert'), may hold values from -0.125 to 0.125
- w_shared_out: bfloat16 [2816, 2048], P('expert'), may hold values from -0.109375 to 0.109375
- w_expert_in: bfloat16 [16, 2, 1408, 2048], P('expert', None, ('dp', 'ctx')), may hold values from -0.125 to 0.125
- w_expert_out: bfloat16 [16, 1408, 2048], P('expert', ('dp', 'ctx')), may hold values from -2.5 to 2.5
Outputs:
- layer_output: bfloat16 [16, 256, 2048], P(('dp', 'expert'), 'ctx')
- grad_input: bfloat16 [16, 256, 2048], P(('dp', 'expert'), 'ctx')
- grad_attn_gain: float32 [2048], P('expert')
- grad_w_query: float32 [2048, 3072], P('expert')
- grad_w_latent: float32 [2048, 576], P('expert')
- grad_latent_gain: float32 [512], P('expert')
- grad_w_expand: float32 [512, 4096], P('expert')
- grad_w_output: float32 [2048, 2048], P('expert')
- grad_ffn_gain: float32 [2048], P('expert')
- grad_w_router: float32 [2048, 16], P('expert')
- grad_w_shared_in: float32 [2048, 5632], P('expert')
- grad_w_shared_out: float32 [2816, 2048], P('expert')
- grad_w_expert_in: float32 [16, 2, 1408, 2048], P('expert', None, ('dp', 'ctx'))
- grad_w_expert_out: float32 [16, 1408, 2048], P('expert', ('dp', 'ctx'))
The draws below stay inside these ranges and needn't reach their ends.
Inputs may be any that keep to these rules, and one draw needn't show every extreme that they name: `routes`: each token names 6 different experts; among the 128 tokens of one device no expert is named more than 64 times, a bound that some block reaches.
All inputs are finite; a program needn't handle non-finite values.
Results may differ from the reference program's by a relative error of at most 0.028.
Values may be sent and summed in bfloat16 or wider, within the bound.
A program may use at most 384 MiB of HBM per device.

```python
import math
import jax
import jax.numpy as jnp
import numpy as np
from jax import lax

D = 2048
HEADS = 16
NOPE = 128
ROPE = 64
VH = 128
KV = 512
EFF = 1408
SHARED = 2
TOP = 6
TOK_DEV = 128
EXPERTS = 16
CAP = 64
SEQS = 16
LENGTH = 256
N_CTX = 2


def level_of(stream_key, dims, split, low, largest):
    loudness = 1.0
    for dim, parts in split:
        steps = jax.random.uniform(jax.random.fold_in(jax.random.fold_in(stream_key, 6), dim), (parts,), jnp.float32, low / len(split), largest / len(split))
        loudness = loudness * jnp.repeat(jnp.exp(steps), dims[dim] // parts).reshape((-1,) + (1,) * (len(dims) - 1 - dim))
    return loudness


def deal_out(stream_key, own, number, rows, number_of, top, reach, slope):
    ranking = jax.random.permutation(stream_key, number_of)
    heavy_load, ordinary = shares(number_of, rows * top, reach, slope, True), shares(number_of, rows * top, reach, slope, False)
    places = jnp.arange(number_of)

    def named(lengths, rotation):
        used = int((lengths > 0).sum())
        fixed = max(1, used // 4)
        shifted = fixed + (places - fixed + rotation * (used - fixed)) % max(1, number_of - fixed)
        return jnp.zeros((number_of,), jnp.int32).at[ranking[jnp.where(places < fixed, places, shifted)]].set(jnp.asarray(lengths, jnp.int32))

    lengths = jnp.where(number % 4 == 0, named(heavy_load, number // 4), named(ordinary, number - number // 4 - 1))
    mixed = jax.random.permutation(jax.random.fold_in(own, 3), number_of)
    source_of, receiver = mixed[0:number_of // 2 * 2:2], mixed[1:number_of // 2 * 2:2]
    room = jnp.minimum(lengths[source_of] - 1, reach - lengths[receiver]) // 2
    room = jnp.where((source_of == ranking[0]) | (receiver == ranking[0]) | (lengths[receiver] == 0), 0, jnp.maximum(room, 0))
    shifted = jax.random.randint(jax.random.fold_in(own, 4), (number_of // 2,), 0, 1 << 20) % (room + 1)
    lengths = lengths.at[source_of].add(-shifted).at[receiver].add(shifted)
    items = jnp.searchsorted(jnp.cumsum(lengths), jnp.arange(rows * top), side="right").astype(jnp.int32)
    table = items.reshape(top, rows).T
    table = table[jax.random.permutation(jax.random.fold_in(own, 1), rows)]
    rotation = jax.random.randint(jax.random.fold_in(own, 2), (rows, 1), 0, top)
    return jnp.take_along_axis(table, (jnp.arange(top)[None, :] + rotation) % top, axis=1)


def shares(amount, total, limit, skew, full):
    portions = [(1 << 20) // math.isqrt(standing ** skew) + 1 for standing in range(1, amount + 1)]
    largest = limit if full else min(limit, max(-(-total // amount), total * portions[0] // sum(portions)))
    least = 1 if total - largest >= amount - 1 else 0
    holding, spare = [largest] + [least] * (amount - 1), total - largest - least * (amount - 1)
    while spare > 0:
        free = [i for i in range(1, amount) if holding[i] < largest] or [i for i in range(1, amount) if holding[i] < limit]
        mass, budget = sum([portions[i] for i in free]), spare
        for i in free:
            addition = min(limit - holding[i], max(1, budget * portions[i] // mass), spare)
            holding[i] = holding[i] + addition
            spare = spare - addition
    return np.array(holding)


def normal_values(stream_key, shape, deviation, reach, pieces=(), held_as=jnp.bfloat16):
    factor_of = level_of(stream_key, shape, pieces, -0.22, 0.18) if pieces else 1.0
    drawn = jax.random.normal(stream_key, shape, jnp.float32) * deviation * factor_of
    return jnp.minimum(jnp.maximum(drawn, -reach), reach).astype(held_as)


def setup_inputs(seed: int = 0) -> dict:
    key_of = jax.random.split(jax.random.key(seed), 16)
    layer_input = normal_values(key_of[0], (SEQS, LENGTH, D), 1.0, 6.0, ((0, 16), (1, 2)))
    cotangent = normal_values(key_of[1], (SEQS, LENGTH, D), 1.0, 6.0, ((0, 16), (1, 2)))
    routes_keys = jax.random.split(jax.random.fold_in(key_of[2], 1), SEQS * LENGTH // TOK_DEV)
    routes_turns = jax.random.permutation(jax.random.fold_in(key_of[2], 3), SEQS * LENGTH // TOK_DEV)
    routes = jax.vmap(lambda own, number: deal_out(jax.random.fold_in(key_of[2], 2), own, number, TOK_DEV, EXPERTS, TOP, CAP, 2))(routes_keys, routes_turns).reshape((SEQS, LENGTH, TOP))
    attn_gain = jnp.clip(1.0 + 0.1 * jax.random.normal(key_of[3], (D,), jnp.float32), 0.5, 1.5)
    w_query = normal_values(key_of[4], (D, HEADS * (NOPE + ROPE)), D ** -0.5, 0.125, ((0, 8),))
    w_latent = normal_values(key_of[5], (D, KV + ROPE), D ** -0.5, 0.125, ((0, 8),))
    latent_gain = jnp.clip(1.0 + 0.1 * jax.random.normal(key_of[6], (KV,), jnp.float32), 0.5, 1.5)
    w_expand = normal_values(key_of[7], (KV, HEADS * (NOPE + VH)), KV ** -0.5, 0.25, ((0, 8),))
    w_output = normal_values(key_of[8], (HEADS * VH, D), (HEADS * VH // 16) ** -0.5, 0.5, ((0, 8),))
    ffn_gain = jnp.clip(1.0 + 0.1 * jax.random.normal(key_of[9], (D,), jnp.float32), 0.5, 1.5)
    w_router = normal_values(key_of[10], (D, EXPERTS), D ** -0.5, 0.125, ((0, 8),))
    w_shared_in = normal_values(key_of[11], (D, 2 * SHARED * EFF), D ** -0.5, 0.125, ((0, 8),))
    w_shared_out = normal_values(key_of[12], (SHARED * EFF, D), (SHARED * EFF) ** -0.5, 0.109375, ((0, 8),))
    w_expert_in = normal_values(key_of[13], (EXPERTS, 2, EFF, D), D ** -0.5, 0.125, ((0, 8), (2, 4)))
    w_expert_out = normal_values(key_of[14], (EXPERTS, EFF, D), (max(EFF // 256, 1)) ** -0.5, 2.5, ((0, 8), (1, 4)))
    return dict(layer_input=layer_input, cotangent=cotangent, routes=routes, attn_gain=attn_gain, w_query=w_query, w_latent=w_latent, latent_gain=latent_gain, w_expand=w_expand, w_output=w_output, ffn_gain=ffn_gain, w_router=w_router, w_shared_in=w_shared_in, w_shared_out=w_shared_out, w_expert_in=w_expert_in, w_expert_out=w_expert_out)


EPS = 1e-06
PRECISE = lax.Precision.HIGHEST

@jax.custom_vjp
def low(v):
    return lax.optimization_barrier(v.astype(jnp.bfloat16)).astype(jnp.float32)

@jax.custom_vjp
def low_back(v):
    return v

def low_keep(v):
    return (low(v), None)

def low_pass(kept, grad):
    return (grad,)

def back_keep(v):
    return (v, None)

def back_low(kept, grad):
    return (low(grad),)
low.defvjp(low_keep, low_pass)
low_back.defvjp(back_keep, back_low)

def matmul(left_side, right_side):
    return jnp.dot(left_side, right_side, precision=PRECISE)

def norm_rows(operand, gain_row):
    return operand * lax.rsqrt(lax.optimization_barrier(jnp.mean(operand * operand, axis=-1, keepdims=True)) + EPS) * gain_row

def rotate(operand, cosine, sine_part):
    half_width = operand.shape[-1] // 2
    former = operand[..., :half_width]
    latter = operand[..., half_width:]
    return jnp.concatenate([former * cosine - latter * sine_part, latter * cosine + former * sine_part], axis=-1)

def softmax_rows(scores):
    highest = lax.optimization_barrier(jnp.max(scores, axis=-1, keepdims=True))
    exponent = jnp.exp(scores - highest)
    return exponent / lax.optimization_barrier(jnp.sum(exponent, axis=-1, keepdims=True))

def attend(queries, compressed, key_rope, offset, w_expand):
    length = compressed.shape[0]
    row_count = queries.shape[0]
    expanded = low(low_back(matmul(compressed, w_expand))).reshape(length, HEADS, NOPE + VH)
    scores = jnp.einsum('qhd,khd->hqk', queries[..., :NOPE], expanded[..., :NOPE], precision=PRECISE)
    scores = scores + jnp.einsum('qhd,kd->hqk', queries[..., NOPE:], key_rope, precision=PRECISE)
    scores = low_back(scores * (1.0 / math.sqrt(NOPE + ROPE)))
    places = offset * row_count + jnp.arange(row_count, dtype=jnp.int32)
    allowed = jnp.arange(length, dtype=jnp.int32)[None, :] <= places[:, None]
    scores = jnp.where(allowed[None], scores, -1e+30)
    weights = low(softmax_rows(scores))
    return jnp.einsum('hqk,khd->qhd', weights, expanded[..., NOPE:], precision=PRECISE)

def expert_rows(row_block, gate_up, down_weight):
    paired = low_back(jnp.einsum('md,gfd->mgf', row_block, gate_up, precision=PRECISE))
    action = low(jax.nn.silu(paired[:, 0]) * paired[:, 1])
    return low(low_back(matmul(action, down_weight)))

def place_slots(block_routes):
    picked_ids = block_routes.reshape(-1)
    onehot = (picked_ids[:, None] == jnp.arange(EXPERTS, dtype=jnp.int32)[None, :]).astype(jnp.int32)
    position = lax.optimization_barrier(jnp.sum((jnp.cumsum(onehot, axis=0) - onehot) * onehot, axis=1))
    target = (picked_ids * CAP + position).astype(jnp.int32)
    assigns = picked_ids.shape[0]
    holder = jnp.full((EXPERTS * CAP,), assigns, jnp.int32).at[target].set(jnp.arange(assigns, dtype=jnp.int32))
    return (target, holder)

def take_rows(source_table, indices):
    return source_table[indices]

def reference(layer_input, cotangent, routes, attn_gain, w_query, w_latent, latent_gain, w_expand, w_output, ffn_gain, w_router, w_shared_in, w_shared_out, w_expert_in, w_expert_out):
    blocks = SEQS * N_CTX
    target, holder = jax.vmap(place_slots)(routes.reshape(blocks, TOK_DEV, TOP))
    offsets = jnp.arange(blocks, dtype=jnp.int32) % N_CTX
    positions = jnp.tile(jnp.arange(LENGTH, dtype=jnp.int32), SEQS).astype(jnp.float32)
    inverse = 10000.0 ** (-jnp.arange(0, ROPE, 2).astype(jnp.float32) / ROPE)
    angles = positions[:, None] * inverse[None, :]
    cosine = jnp.cos(angles)
    sine_part = jnp.sin(angles)
    flat_routes = routes.reshape(-1, TOP)

    def forward(inputs, g_attn, weight_query, weight_latent, g_latent, weight_expand, weight_output, g_ffn, weight_router, weight_shared_in, weight_shared_out, weight_expert_in, weight_expert_out):
        tokens = inputs.reshape(-1, D)
        hidden_one = low(norm_rows(tokens, g_attn))
        queries = low_back(matmul(hidden_one, weight_query)).reshape(-1, HEADS, NOPE + ROPE)
        queries = low(jnp.concatenate([queries[..., :NOPE], rotate(queries[..., NOPE:], cosine[:, None, :], sine_part[:, None, :])], axis=-1))
        latent = low_back(matmul(hidden_one, weight_latent))
        compressed = low(norm_rows(latent[:, :KV], g_latent))
        key_rope = low(rotate(latent[:, KV:], cosine, sine_part))
        comp_seq = jnp.repeat(compressed.reshape(SEQS, LENGTH, KV), N_CTX, axis=0)
        rope_seq = jnp.repeat(key_rope.reshape(SEQS, LENGTH, ROPE), N_CTX, axis=0)

        def one_block(block_item):
            return attend(block_item[0], block_item[1], block_item[2], block_item[3], weight_expand)
        mixed_heads = lax.map(jax.checkpoint(one_block), (queries.reshape(blocks, TOK_DEV, HEADS, NOPE + ROPE), comp_seq, rope_seq, offsets))
        mixed_heads = low(low_back(mixed_heads.reshape(-1, HEADS * VH)))
        first_sum = tokens + low_back(matmul(mixed_heads, weight_output))
        hidden_two = low(norm_rows(first_sum, g_ffn))
        router = softmax_rows(low_back(matmul(hidden_two, weight_router)))
        picked = jnp.take_along_axis(router, flat_routes, axis=1)
        shared_gu = low_back(matmul(hidden_two, weight_shared_in))
        shared_act = low(jax.nn.silu(shared_gu[:, :SHARED * EFF]) * shared_gu[:, SHARED * EFF:])
        shared = low_back(matmul(shared_act, weight_shared_out))
        padded = jnp.concatenate([hidden_two.reshape(blocks, TOK_DEV, D), jnp.zeros((blocks, 1, D), jnp.float32)], axis=1)
        rows_in = low_back(jax.vmap(take_rows)(padded, holder // TOP))
        rows_in = rows_in.reshape(blocks, EXPERTS, CAP, D).transpose(1, 0, 2, 3).reshape(EXPERTS, blocks * CAP, D)

        def one_expert(expert_item):
            return expert_rows(expert_item[0], expert_item[1], expert_item[2])
        results = lax.map(jax.checkpoint(one_expert), (rows_in, weight_expert_in, weight_expert_out))
        results = results.reshape(EXPERTS, blocks, CAP, D).transpose(1, 0, 2, 3).reshape(blocks, EXPERTS * CAP, D)
        taken = jax.vmap(take_rows)(results, target).reshape(-1, TOP, D)
        routed = lax.optimization_barrier(jnp.sum(picked[:, :, None] * taken, axis=1))
        return (first_sum + shared + routed).reshape(SEQS, LENGTH, D)
    primal, pullback = jax.vjp(forward, layer_input.astype(jnp.float32), attn_gain, w_query.astype(jnp.float32), w_latent.astype(jnp.float32), latent_gain, w_expand.astype(jnp.float32), w_output.astype(jnp.float32), ffn_gain, w_router.astype(jnp.float32), w_shared_in.astype(jnp.float32), w_shared_out.astype(jnp.float32), w_expert_in.astype(jnp.float32), w_expert_out.astype(jnp.float32))
    gradients = pullback(cotangent.astype(jnp.float32))
    return (primal.astype(jnp.bfloat16), gradients[0].astype(jnp.bfloat16), gradients[1], gradients[2], gradients[3], gradients[4], gradients[5], gradients[6], gradients[7], gradients[8], gradients[9], gradients[10], gradients[11], gradients[12])
```

```python
import functools
import math

import jax
import jax.numpy as jnp
from jax import lax
from jax.experimental import pallas as pl
from jax.experimental.pallas import tpu as pltpu
from jax.sharding import PartitionSpec as P

HEADS = 16
NOPE = 128
ROPE = 64
VH = 128
KV = 512
TOP = 6


EPS = 1e-06

MESH = pl.DeviceIdType.MESH
ALL = ("dp", "ctx", "expert")
PLANE = ("dp", "ctx")
BF = jnp.bfloat16
F32 = jnp.float32
LANES = 128
CHUNK = 512
VMEM_LIMIT = 66_000_000


def here():
    spot = lax.axis_index("expert")
    return lax.axis_index("dp"), lax.axis_index("ctx"), spot // 2, lax.rem(spot, 2)


def greet(peers):
    barrier = pltpu.get_barrier_semaphore()
    for peer in peers:
        pl.semaphore_signal(barrier, inc=1, device_id=peer, device_id_type=MESH)
    pl.semaphore_wait(barrier, len(peers))


class Sends:
    def __init__(self, sems):
        self.sems, self.started = sems, []

    def go(self, src, dst, arrival, peer):
        copy = pltpu.make_async_remote_copy(
            src_ref=src,
            dst_ref=dst,
            send_sem=self.sems.at[len(self.started)],
            recv_sem=arrival,
            device_id=peer,
            device_id_type=MESH,
        )
        copy.start()
        self.started.append(copy)

    def drain(self):
        for copy in self.started:
            copy.wait_send()


def arrive(ref, sem, peer):
    pltpu.make_async_remote_copy(
        src_ref=ref, dst_ref=ref, send_sem=sem, recv_sem=sem, device_id=peer, device_id_type=MESH
    ).wait_recv()


def gather_all_kernel(nz, rows, own, out, lsem, ssem, zsem, xsem, ysem, dasem, dbsem, csem):
    x, y, z, c = here()
    half = rows // 2
    first, second = pl.ds(0, half), pl.ds(half, half)
    xn, yn, cn = (1 - x, y, 2 * z + c), (x, 1 - y, 2 * z + c), (x, y, 2 * z + 1 - c)
    source = [lax.rem(z + nz - k, nz) for k in range(nz)]
    zpeers = [(x, y, 2 * lax.rem(z + k, nz) + c) for k in range(1, nz)]
    greet(zpeers + [xn, yn, cn])
    sends = Sends(ssem)
    mine = out.at[x, y, z, c]
    for k in range(1, nz):
        sends.go(own, mine, zsem.at[k], zpeers[k - 1])
    local = pltpu.make_async_copy(own, mine, lsem)
    local.start()

    def column(j, src):
        dst = out.at[x, y, source[j], c]
        sends.go(src, dst, xsem.at[j], xn)
        sends.go(src, dst, ysem.at[j], yn)
        sends.go(src, dst, csem.at[j], cn)

    def sides(j):
        part = out.at[1 - x, y, source[j], c]
        arrive(part, xsem.at[j], xn)
        sends.go(part.at[first], part.at[first], dasem.at[j], yn)
        sends.go(part, part, csem.at[nz + j], cn)
        part = out.at[x, 1 - y, source[j], c]
        arrive(part, ysem.at[j], yn)
        sends.go(part.at[second], part.at[second], dbsem.at[j], xn)
        sends.go(part, part, csem.at[2 * nz + j], cn)

    def corner(j):
        part = out.at[1 - x, 1 - y, source[j], c]
        arrive(part.at[first], dasem.at[j], yn)
        arrive(part.at[second], dbsem.at[j], xn)
        sends.go(part, part, csem.at[3 * nz + j], cn)

    column(0, own)
    for step in range(1, nz + 2):
        if step < nz:
            part = out.at[x, y, source[step], c]
            arrive(part, zsem.at[step], zpeers[0])
            column(step, part)
        if step - 1 < nz:
            sides(step - 1)
        if 0 <= step - 2 < nz:
            corner(step - 2)
    for q, (qx, qy) in enumerate(((x, y), (1 - x, y), (x, 1 - y), (1 - x, 1 - y))):
        for j in range(nz):
            arrive(out.at[qx, qy, source[j], 1 - c], csem.at[q * nz + j], cn)
    sends.drain()
    local.wait()


def gather_all(own, nz, number):
    rows, width = own.shape
    dma = pltpu.SemaphoreType.DMA
    return pl.pallas_call(
        functools.partial(gather_all_kernel, nz, rows),
        out_shape=jax.ShapeDtypeStruct((2, 2, nz, 2, rows, width), own.dtype),
        in_specs=[pl.BlockSpec(memory_space=pltpu.VMEM)],
        out_specs=pl.BlockSpec(memory_space=pl.ANY),
        scratch_shapes=[
            dma(()),
            dma((9 * nz - 1,)),
            dma((nz,)),
            dma((nz,)),
            dma((nz,)),
            dma((nz,)),
            dma((nz,)),
            dma((4 * nz,)),
        ],
        compiler_params=pltpu.CompilerParams(collective_id=number, has_side_effects=True),
        name=f"gather_all_{number}",
    )(own)


def sum_all_kernel(
    nz, rows, part, out, own, rc, rda, rdb, rx, ry, rz, lsem, ssem, csem, dasem, dbsem, xsem, ysem, zsem
):
    x, y, z, c = here()
    half = rows // 2
    first, second = pl.ds(0, half), pl.ds(half, half)
    xn, yn, cn = (1 - x, y, 2 * z + c), (x, 1 - y, 2 * z + c), (x, y, 2 * z + 1 - c)
    dest = [lax.rem(z + 1 + i, nz) for i in range(nz)]
    zpeers = [(x, y, 2 * dest[i] + c) for i in range(nz - 1)]
    greet(zpeers + [xn, yn, cn])
    sends = Sends(ssem)
    quads = ((1 - x, 1 - y), (1 - x, y), (x, 1 - y), (x, y))
    loads = {}
    for i in range(nz):
        for q, (qx, qy) in enumerate(quads):
            sends.go(part.at[qx, qy, dest[i], 1 - c], rc.at[q, i], csem.at[q * nz + i], cn)
            loads[q, i] = pltpu.make_async_copy(
                part.at[qx, qy, dest[i], c], own.at[q, i], lsem.at[q * nz + i]
            )
            loads[q, i].start()

    def base(q, i):
        loads[q, i].wait()
        arrive(rc.at[q, i], csem.at[q * nz + i], cn)

    def val(ref):
        return ref[...].astype(F32)

    def corner(i):
        base(0, i)
        own[0, i] = (val(own.at[0, i]) + val(rc.at[0, i])).astype(BF)
        sends.go(own.at[0, i, first], rda.at[i], dasem.at[i], yn)
        sends.go(own.at[0, i, second], rdb.at[i], dbsem.at[i], xn)

    def sides(i):
        base(1, i)
        own[1, i, second] = (val(own.at[1, i, second]) + val(rc.at[1, i, second])).astype(BF)
        arrive(rda.at[i], dasem.at[i], yn)
        own[1, i, first] = (
            val(own.at[1, i, first]) + val(rc.at[1, i, first]) + val(rda.at[i])
        ).astype(BF)
        sends.go(own.at[1, i], rx.at[i], xsem.at[i], xn)
        base(2, i)
        own[2, i, first] = (val(own.at[2, i, first]) + val(rc.at[2, i, first])).astype(BF)
        arrive(rdb.at[i], dbsem.at[i], xn)
        own[2, i, second] = (
            val(own.at[2, i, second]) + val(rc.at[2, i, second]) + val(rdb.at[i])
        ).astype(BF)
        sends.go(own.at[2, i], ry.at[i], ysem.at[i], yn)

    def column(i):
        base(3, i)
        arrive(rx.at[i], xsem.at[i], xn)
        arrive(ry.at[i], ysem.at[i], yn)
        total = val(own.at[3, i]) + val(rc.at[3, i]) + val(rx.at[i]) + val(ry.at[i])
        if i < nz - 1:
            own[3, i] = total.astype(BF)
            sends.go(own.at[3, i], rz.at[i], zsem.at[i], zpeers[i])
        else:
            for k in range(nz - 1):
                arrive(rz.at[k], zsem.at[k], zpeers[0])
                total = total + val(rz.at[k])
            out[...] = total

    for step in range(nz + 2):
        if step < nz:
            corner(step)
        if 0 <= step - 1 < nz:
            sides(step - 1)
        if 0 <= step - 2 < nz:
            column(step - 2)
    sends.drain()


def sum_all(part, nz, number):
    rows, width = part.shape[-2:]
    dma = pltpu.SemaphoreType.DMA

    def space(*dims):
        return pltpu.VMEM(dims + (width,), BF)

    return pl.pallas_call(
        functools.partial(sum_all_kernel, nz, rows),
        out_shape=jax.ShapeDtypeStruct((rows, width), F32),
        in_specs=[pl.BlockSpec(memory_space=pl.ANY)],
        out_specs=pl.BlockSpec(memory_space=pltpu.VMEM),
        scratch_shapes=[
            space(4, nz, rows),
            space(4, nz, rows),
            space(nz, rows // 2),
            space(nz, rows // 2),
            space(nz, rows),
            space(nz, rows),
            space(nz - 1, rows),
            dma((4 * nz,)),
            dma((9 * nz - 1,)),
            dma((4 * nz,)),
            dma((nz,)),
            dma((nz,)),
            dma((nz,)),
            dma((nz,)),
            dma((nz - 1,)),
        ],
        compiler_params=pltpu.CompilerParams(
            collective_id=number, has_side_effects=True, vmem_limit_bytes=VMEM_LIMIT
        ),
        name=f"sum_all_{number}",
    )(part)


def gather_plane_kernel(rows, own, out, lsem, ssem, rsem):
    x, y, z, c = here()
    half = rows // 2
    first, second = pl.ds(0, half), pl.ds(half, half)
    xn, yn = (1 - x, y, 2 * z + c), (x, 1 - y, 2 * z + c)
    greet([xn, yn])
    sends = Sends(ssem)
    mine = out.at[x, y]
    sends.go(own, mine, rsem.at[0], xn)
    sends.go(own, mine, rsem.at[1], yn)
    local = pltpu.make_async_copy(own, mine, lsem)
    local.start()
    part = out.at[1 - x, y]
    arrive(part, rsem.at[0], xn)
    sends.go(part.at[first], part.at[first], rsem.at[2], yn)
    part = out.at[x, 1 - y]
    arrive(part, rsem.at[1], yn)
    sends.go(part.at[second], part.at[second], rsem.at[3], xn)
    part = out.at[1 - x, 1 - y]
    arrive(part.at[first], rsem.at[2], yn)
    arrive(part.at[second], rsem.at[3], xn)
    sends.drain()
    local.wait()


def gather_plane(own, number):
    rows, width = own.shape
    dma = pltpu.SemaphoreType.DMA
    return pl.pallas_call(
        functools.partial(gather_plane_kernel, rows),
        out_shape=jax.ShapeDtypeStruct((2, 2, rows, width), own.dtype),
        in_specs=[pl.BlockSpec(memory_space=pltpu.VMEM)],
        out_specs=pl.BlockSpec(memory_space=pltpu.VMEM),
        scratch_shapes=[dma(()), dma((4,)), dma((4,))],
        compiler_params=pltpu.CompilerParams(collective_id=number, has_side_effects=True),
        name=f"gather_plane_{number}",
    )(own)


def swap_plane_kernel(part, out, lsem, ssem, rsem):
    x, y, z, c = here()
    spots = ((1 - x, y), (x, 1 - y), (1 - x, 1 - y))
    peers = [(px, py, 2 * z + c) for px, py in spots]
    greet(peers)
    sends = Sends(ssem)
    for k, (px, py) in enumerate(spots):
        sends.go(part.at[px, py], out.at[x, y], rsem.at[k], peers[k])
    local = pltpu.make_async_copy(part.at[x, y], out.at[x, y], lsem)
    local.start()
    for k, (px, py) in enumerate(spots):
        arrive(out.at[px, py], rsem.at[k], peers[k])
    sends.drain()
    local.wait()


def swap_plane(part, number):
    dma = pltpu.SemaphoreType.DMA
    return pl.pallas_call(
        swap_plane_kernel,
        out_shape=jax.ShapeDtypeStruct(part.shape, part.dtype),
        in_specs=[pl.BlockSpec(memory_space=pltpu.VMEM)],
        out_specs=pl.BlockSpec(memory_space=pltpu.VMEM),
        scratch_shapes=[dma(()), dma((3,)), dma((3,))],
        compiler_params=pltpu.CompilerParams(collective_id=number, has_side_effects=True),
        name=f"swap_plane_{number}",
    )(part)


def sum_plane_kernel(rows, part, out, rda, rdb, rx, ry, sx, sy, ssem, rsem):
    x, y, z, c = here()
    half = rows // 2
    first, second = pl.ds(0, half), pl.ds(half, half)
    xn, yn = (1 - x, y, 2 * z + c), (x, 1 - y, 2 * z + c)
    greet([xn, yn])
    sends = Sends(ssem)
    corner, xside, yside = part.at[1 - x, 1 - y], part.at[1 - x, y], part.at[x, 1 - y]
    sends.go(corner.at[first], rda, rsem.at[0], yn)
    sends.go(corner.at[second], rdb, rsem.at[1], xn)
    sends.go(xside.at[second], rx.at[second], rsem.at[2], xn)
    sends.go(yside.at[first], ry.at[first], rsem.at[3], yn)
    arrive(rda, rsem.at[0], yn)
    sx[...] = (xside[first].astype(F32) + rda[...].astype(F32)).astype(BF)
    sends.go(sx, rx.at[first], rsem.at[4], xn)
    arrive(rdb, rsem.at[1], xn)
    sy[...] = (yside[second].astype(F32) + rdb[...].astype(F32)).astype(BF)
    sends.go(sy, ry.at[second], rsem.at[5], yn)
    arrive(rx.at[second], rsem.at[2], xn)
    arrive(ry.at[first], rsem.at[3], yn)
    arrive(rx.at[first], rsem.at[4], xn)
    arrive(ry.at[second], rsem.at[5], yn)
    out[...] = part[x, y].astype(F32) + rx[...].astype(F32) + ry[...].astype(F32)
    sends.drain()


def sum_plane(part, number):
    rows, width = part.shape[-2:]
    dma = pltpu.SemaphoreType.DMA

    def space(count):
        return pltpu.VMEM((count, width), BF)

    return pl.pallas_call(
        functools.partial(sum_plane_kernel, rows),
        out_shape=jax.ShapeDtypeStruct((rows, width), F32),
        in_specs=[pl.BlockSpec(memory_space=pltpu.VMEM)],
        out_specs=pl.BlockSpec(memory_space=pltpu.VMEM),
        scratch_shapes=[
            space(rows // 2),
            space(rows // 2),
            space(rows),
            space(rows),
            space(rows // 2),
            space(rows // 2),
            dma((6,)),
            dma((6,)),
        ],
        compiler_params=pltpu.CompilerParams(collective_id=number, has_side_effects=True),
        name=f"sum_plane_{number}",
    )(part)


def dot_nn(left, right):
    return lax.dot_general(left, right, (((1,), (0,)), ((), ())), preferred_element_type=F32)


def dot_nt(left, right):
    return lax.dot_general(left, right, (((1,), (1,)), ((), ())), preferred_element_type=F32)


def dot_tn(left, right):
    return lax.dot_general(left, right, (((0,), (0,)), ((), ())), preferred_element_type=F32)


def silu_parts(operand):
    sigmoid_of = jax.nn.sigmoid(operand)
    return (operand * sigmoid_of, sigmoid_of * (1.0 + operand * (1.0 - sigmoid_of)))


def ffn_kernel(
    dims,
    h,
    g,
    pos,
    win,
    wout,
    wcat,
    wso,
    out,
    gh,
    o_gwin,
    o_gwout,
    o_gwcat,
    o_gwso,
    rows,
    grows,
    gwin,
    gwout,
    gwcat,
    gwso,
    osem,
):
    hidden, padded, slots, shared, experts = dims
    step = pl.program_id(0)
    tokens, width = h.shape
    block = 2 * LANES
    pairs = tokens // block
    per = 2 * slots
    first_lane = shared + 2 * lax.axis_index("expert")

    @pl.when(step == 0)
    def _():
        gwin[...] = jnp.zeros_like(gwin)
        gwout[...] = jnp.zeros_like(gwout)
        gwcat[...] = jnp.zeros_like(gwcat)
        gwso[...] = jnp.zeros_like(gwso)

    def chunks(body):
        def run(n, carry):
            body(pl.ds(pl.multiple_of(n * CHUNK, CHUNK), CHUNK))
            return carry

        lax.fori_loop(0, width // CHUNK, run, 0)

    mixed = dot_nn(h[...], wcat[...])
    gate, up = mixed[:, :LANES], mixed[:, LANES:]
    lane = lax.broadcasted_iota(jnp.int32, gate.shape, 1)
    of_router = (lane >= shared) & (lane < shared + experts)
    logits = jnp.where(of_router, gate, -1e30)
    raised = jnp.where(of_router, jnp.exp(logits - jnp.max(logits, axis=1, keepdims=True)), 0.0)
    router = raised / jnp.sum(raised, axis=1, keepdims=True)
    silu, slope = silu_parts(gate)
    act = (silu * up).astype(BF)
    gact = dot_nt(g[...], wso[...])
    ggate = gact * up * slope
    gup = gact * silu
    high = router.astype(BF)
    router_parts = jnp.concatenate([high, (router - high.astype(F32)).astype(BF)], axis=1)
    slot_lane = lax.broadcasted_iota(jnp.int32, (per, LANES), 1)
    slot_row = lax.broadcasted_iota(jnp.int32, (per, block), 0)
    picks, picked = [], [[], []]
    for pair in range(pairs):
        span = slice(pair * block, (pair + 1) * block)
        pick = jnp.concatenate(
            [
                jnp.where(pos[j : j + 1, span] == slot_row, 1.0, 0.0).astype(BF) for j in range(2)
            ],
            axis=0,
        )
        picks.append(pick)
        place = slice(pair * per, (pair + 1) * per)

        def fetch(cols, pick=pick, span=span, place=place):
            taken = dot_nn(pick, h[span, cols]).astype(BF)
            rows[0, place, cols] = taken[:per]
            rows[1, place, cols] = taken[per:]
            taken = dot_nn(pick, g[span, cols]).astype(BF)
            grows[0, place, cols] = taken[:per]
            grows[1, place, cols] = taken[per:]

        chunks(fetch)
        taken = dot_nn(pick, router_parts[span])
        taken = taken[:, :LANES] + taken[:, LANES:]
        for j in range(2):
            picked[j].append(
                jnp.sum(
                    jnp.where(slot_lane == first_lane + j, taken[j * per : (j + 1) * per], 0.0),
                    axis=1,
                    keepdims=True,
                )
            )
    grad_picked = []
    for j in range(2):
        share = jnp.concatenate(picked[j], axis=0)
        both = dot_nt(rows[j], win[j])
        egate, eup = both[:, :padded], both[:, padded:]
        raw = dot_nt(grows[j], wout[j])
        esilu, eslope = silu_parts(egate)
        eact = esilu * eup
        grad_picked.append(jnp.sum(eact * raw, axis=1, keepdims=True))
        scaled = (share * eact).astype(BF)
        graw = share * raw
        gboth = jnp.concatenate([graw * eup * eslope, graw * esilu], axis=1).astype(BF)

        def expert(cols, j=j, scaled=scaled, gboth=gboth):
            gin, gout = rows[j, :, cols], grows[j, :, cols]
            gwout[j, :, cols] += dot_tn(scaled[:, :hidden], gout)
            gwin[j, 0, :, cols] += dot_tn(gboth[:, :hidden], gin)
            gwin[j, 1, :, cols] += dot_tn(gboth[:, padded : padded + hidden], gin)
            grows[j, :, cols] = dot_nn(scaled, wout[j, :, cols]).astype(BF)
            rows[j, :, cols] = dot_nn(gboth, win[j, :, cols]).astype(BF)

        chunks(expert)
    gparts = []
    for pair in range(pairs):
        span = slice(pair * block, (pair + 1) * block)
        place = slice(pair * per, (pair + 1) * per)
        pick = picks[pair]
        spread = jnp.concatenate(
            [
                jnp.where(slot_lane == first_lane + j, grad_picked[j][place], 0.0)
                for j in range(2)
            ],
            axis=0,
        )
        high = spread.astype(BF)
        low = (spread - high.astype(F32)).astype(BF)
        grouter = dot_tn(pick, jnp.concatenate([high, low], axis=1))
        grouter = grouter[:, :LANES] + grouter[:, LANES:]
        share = router[span]
        glogits = share * (grouter - jnp.sum(share * grouter, axis=1, keepdims=True))
        gpart = jnp.concatenate([ggate[span] + glogits, gup[span]], axis=1).astype(BF)
        gparts.append(gpart)

        def spreads(cols, pick=pick, span=span, place=place, gpart=gpart):
            sent = jnp.concatenate([grows[0, place, cols], grows[1, place, cols]], axis=0)
            out[span, cols] = (dot_tn(pick, sent) + dot_nn(act[span], wso[:, cols])).astype(BF)
            sent = jnp.concatenate([rows[0, place, cols], rows[1, place, cols]], axis=0)
            gh[span, cols] = (dot_tn(pick, sent) + dot_nt(gpart, wcat[cols, :])).astype(BF)

        chunks(spreads)
    gall = jnp.concatenate(gparts, axis=0)

    def dense(cols):
        gwcat[:, cols] += dot_tn(gall, h[:, cols])
        gwso[:, cols] += dot_tn(act, g[:, cols])

    chunks(dense)

    @pl.when(step == pl.num_programs(0) - 1)
    def _():
        copies = [
            pltpu.make_async_copy(src, dst, osem.at[k])
            for k, (src, dst) in enumerate(
                ((gwin, o_gwin), (gwout, o_gwout), (gwcat, o_gwcat), (gwso, o_gwso))
            )
        ]
        for copy in copies:
            copy.start()
        for copy in copies:
            copy.wait()


def ffn(h, g, pos, win, wout, wcat, wso, hidden, slots, shared, experts):
    count, width = h.shape
    padded = wout.shape[1]
    tokens = 4 * LANES
    whole = pl.Buffered(1)

    def fixed(shape):
        return pl.BlockSpec(shape, lambda i: (0,) * len(shape), pipeline_mode=whole)

    moving = pl.BlockSpec((tokens, width), lambda i: (i, 0))
    left = pl.BlockSpec(memory_space=pl.ANY)
    sums = [(2, 2, hidden, width), (2, hidden, width), (2 * LANES, width), (LANES, width)]
    return pl.pallas_call(
        functools.partial(ffn_kernel, (hidden, padded, slots, shared, experts)),
        grid=(count // tokens,),
        out_shape=[jax.ShapeDtypeStruct((count, width), BF)] * 2
        + [jax.ShapeDtypeStruct(s, F32) for s in sums],
        in_specs=[
            moving,
            moving,
            pl.BlockSpec((8, tokens), lambda i: (0, i)),
            fixed(win.shape),
            fixed(wout.shape),
            fixed(wcat.shape),
            fixed(wso.shape),
        ],
        out_specs=[moving, moving, left, left, left, left],
        scratch_shapes=[
            pltpu.VMEM((2, tokens // LANES * slots, width), BF),
            pltpu.VMEM((2, tokens // LANES * slots, width), BF),
        ]
        + [pltpu.VMEM(s, F32) for s in sums]
        + [pltpu.SemaphoreType.DMA((4,))],
        compiler_params=pltpu.CompilerParams(vmem_limit_bytes=VMEM_LIMIT),
        name="ffn",
    )(h, g, pos, win, wout, wcat, wso)


def head_parts(qn, qf, qs, ex, kf, ks):
    lane = lax.broadcasted_iota(jnp.int32, qf.shape, 1)
    low = pl.program_id(1) * (ROPE // 2)
    mine = (lane >= low) & (lane < low + ROPE // 2)
    zero = jnp.zeros_like(qf[...])
    left = jnp.concatenate(
        [qn[...], jnp.where(mine, qf[...], zero), jnp.where(mine, qs[...], zero)], axis=1
    )
    right = jnp.concatenate([ex[:, :NOPE], kf[...], ks[...]], axis=1)
    scores = dot_nt(left, right) * (1.0 / math.sqrt(NOPE + ROPE))
    row = lax.broadcasted_iota(jnp.int32, scores.shape, 0)
    col = lax.broadcasted_iota(jnp.int32, scores.shape, 1)
    scores = jnp.where(col <= row, scores, -1e30)
    exponent = jnp.exp(scores - jnp.max(scores, axis=1, keepdims=True))
    probs = exponent / jnp.sum(exponent, axis=1, keepdims=True)
    return left, right, probs, mine


def attend_kernel(qn, qf, qs, ex, kf, ks, mixed):
    probs = head_parts(qn, qf, qs, ex, kf, ks)[2]
    mixed[...] = dot_nn(probs.astype(BF), ex[:, NOPE:]).astype(BF)


def attend_back_kernel(qn, qf, qs, ex, kf, ks, gm, gqn, gqf, gqs, gex, gkf, gks):
    left, right, probs, mine = head_parts(qn, qf, qs, ex, kf, ks)
    scale = 1.0 / math.sqrt(NOPE + ROPE)

    @pl.when(pl.program_id(1) == 0)
    def _():
        for ref in (gqf, gqs, gkf, gks):
            ref[...] = jnp.zeros_like(ref)

    gweights = dot_nt(gm[...], ex[:, NOPE:])
    gscores = probs * (gweights - jnp.sum(probs * gweights, axis=1, keepdims=True))
    gscores = gscores.astype(BF)
    gleft = dot_nn(gscores, right) * scale
    gqn[...] = gleft[:, :NOPE].astype(BF)
    gqf[...] += jnp.where(mine, gleft[:, NOPE : NOPE + LANES], 0.0)
    gqs[...] += jnp.where(mine, gleft[:, NOPE + LANES :], 0.0)
    gright = dot_tn(gscores, left) * scale
    gex[:, :NOPE] = gright[:, :NOPE].astype(BF)
    gkf[...] += gright[:, NOPE : NOPE + LANES]
    gks[...] += gright[:, NOPE + LANES :]
    gex[:, NOPE:] = dot_tn(probs.astype(BF), gm[...]).astype(BF)


def attention_specs(length):
    each = pl.BlockSpec((length, NOPE), lambda b, h: (b, h))
    one = pl.BlockSpec((length, LANES), lambda b, h: (b, 0))
    wide = pl.BlockSpec((length, NOPE + VH), lambda b, h: (b, h))
    return each, one, wide


def attend(qn, qf, qs, ex, kf, ks, length):
    each, one, wide = attention_specs(length)
    return pl.pallas_call(
        attend_kernel,
        grid=(qn.shape[0] // length, qn.shape[1] // NOPE),
        out_shape=jax.ShapeDtypeStruct(qn.shape, BF),
        in_specs=[each, one, one, wide, one, one],
        out_specs=each,
        name="attend",
    )(qn, qf, qs, ex, kf, ks)


def attend_back(qn, qf, qs, ex, kf, ks, gm, length):
    each, one, wide = attention_specs(length)
    return pl.pallas_call(
        attend_back_kernel,
        grid=(qn.shape[0] // length, qn.shape[1] // NOPE),
        out_shape=[
            jax.ShapeDtypeStruct(qn.shape, BF),
            jax.ShapeDtypeStruct(qf.shape, F32),
            jax.ShapeDtypeStruct(qf.shape, F32),
            jax.ShapeDtypeStruct(ex.shape, BF),
            jax.ShapeDtypeStruct(qf.shape, F32),
            jax.ShapeDtypeStruct(qf.shape, F32),
        ],
        in_specs=[each, one, one, wide, one, one, each],
        out_specs=[each, one, one, wide, one, one],
        name="attend_back",
    )(qn, qf, qs, ex, kf, ks, gm)


def normalize(operand):
    factor = lax.rsqrt(jnp.mean(operand * operand, axis=-1, keepdims=True) + EPS)
    return (operand * factor, factor)


def norm_back(grad_out, normed, factor, gain_row):
    inner_sums = grad_out * gain_row
    grad_in = factor * (inner_sums - normed * jnp.mean(inner_sums * normed, axis=-1, keepdims=True))
    return (grad_in, jnp.sum(grad_out * normed, axis=0))


def plane_part(operand, index, axis, parts=4):
    size = operand.shape[axis] // parts
    return lax.dynamic_slice_in_dim(operand, index * size, size, axis=axis)


def columns_of(blocks):
    return jnp.moveaxis(blocks, 0, 1).reshape(blocks.shape[1], -1)


def split_body(
    layer_input,
    cotangent,
    routes,
    attn_gain,
    w_query,
    w_latent,
    latent_gain,
    w_expand,
    w_output,
    ffn_gain,
    w_router,
    w_shared_in,
    w_shared_out,
    w_expert_in,
    w_expert_out,
):
    spot = lax.axis_index("expert")
    place = lax.axis_index("dp") * 2 + lax.axis_index("ctx")
    groups = lax.axis_size("expert")
    nz = groups // 2
    tok_count, width = layer_input.shape[1:]
    length = 2 * tok_count
    devices = 4 * groups
    experts = w_router.shape[1]
    capacity = tok_count * TOP * 4 // (3 * experts)
    local_rows = w_query.shape[0]
    heads = HEADS // 4
    nope_cols, rope_cols = heads * NOPE, heads * ROPE // 2
    query_cols = nope_cols + 2 * rope_cols
    out_cols = width // 4
    hidden = w_expert_out.shape[1]
    padded = -(-hidden // LANES) * LANES
    shared_rows = w_shared_out.shape[0]
    units = shared_rows // 4

    tokens = layer_input[0].astype(F32)
    normed_one, factor_one = normalize(tokens)
    hidden_one = (normed_one * attn_gain).astype(BF)
    h1 = gather_plane(hidden_one, 1).reshape(4 * tok_count, width)
    own_query = plane_part(w_query, place, 1).reshape(local_rows, heads, NOPE + ROPE)
    half = NOPE + ROPE // 2
    attn_pack = jnp.concatenate(
        [
            own_query[:, :, :NOPE].reshape(local_rows, nope_cols),
            own_query[:, :, NOPE:half].reshape(local_rows, rope_cols),
            own_query[:, :, half:].reshape(local_rows, rope_cols),
            plane_part(w_output, place, 1),
            w_latent,
        ],
        axis=1,
    )
    attn_w = lax.all_gather(attn_pack, "expert", axis=0, tiled=True)
    weight_expand = lax.all_gather(plane_part(w_expand, place, 1), "expert", axis=0, tiled=True)
    weight_query = attn_w[:, :query_cols]
    weight_output = attn_w[:, query_cols : query_cols + out_cols].reshape(4, out_cols, out_cols)
    weight_latent = attn_w[:, query_cols + out_cols :]

    all_routes = lax.all_gather(routes[0], ALL, axis=0)
    all_grads = lax.all_gather(cotangent[0], ALL, axis=0, tiled=True)
    offset = (jnp.arange(devices, dtype=jnp.int32) % 2 * capacity)[:, None]
    slots = []
    for j in range(2):
        named = jnp.any(all_routes == 2 * spot + j, axis=2)
        order = jnp.cumsum(named.astype(jnp.int32), axis=1) - 1
        slots.append(jnp.where(named, order + offset, -1).reshape(1, -1))
    slots = jnp.concatenate(slots + [jnp.full((6, slots[0].shape[1]), -1, jnp.int32)], axis=0)
    halves = w_shared_in.reshape(local_rows, 2, groups, 4, units)
    halves = lax.dynamic_index_in_dim(halves, place, axis=3, keepdims=False)
    spare = LANES - units - experts
    shared_pack = jnp.concatenate(
        [
            halves[:, 0],
            jnp.broadcast_to(w_router[:, None, :], (local_rows, groups, experts)),
            jnp.zeros((local_rows, groups, spare), BF),
            halves[:, 1],
            jnp.zeros((local_rows, groups, LANES - units), BF),
        ],
        axis=2,
    )
    weight_shared = lax.all_to_all(
        jnp.moveaxis(shared_pack, 1, 0), "expert", split_axis=0, concat_axis=0, tiled=True
    ).reshape(width, 2 * LANES)
    own_shared_out = jnp.pad(plane_part(w_shared_out, place, 0), ((0, LANES - units), (0, 0)))
    widen = padded - hidden
    expert_in = jnp.pad(w_expert_in, ((0, 0), (0, 0), (0, widen), (0, 0))).reshape(
        2, 2 * padded, width
    )
    expert_down = jnp.pad(w_expert_out, ((0, 0), (0, widen), (0, 0)))

    inverse = 10000.0 ** (-jnp.arange(0, ROPE, 2).astype(F32) / ROPE)
    places = jnp.arange(4 * tok_count, dtype=jnp.int32) % length
    angles = places.astype(F32)[:, None] * inverse[None, :]
    cosine, sine_part = jnp.cos(angles), jnp.sin(angles)
    cosines, sines = jnp.tile(cosine, (1, heads)), jnp.tile(sine_part, (1, heads))
    queries = dot_nn(h1, weight_query)
    query_nope = queries[:, :nope_cols].astype(BF)
    former = queries[:, nope_cols : nope_cols + rope_cols]
    latter = queries[:, nope_cols + rope_cols :]
    query_f = (former * cosines - latter * sines).astype(BF)
    query_s = (latter * cosines + former * sines).astype(BF)
    latent = dot_nn(h1, weight_latent)
    normed_lat, factor_lat = normalize(latent[:, :KV])
    compressed = (normed_lat * latent_gain).astype(BF)
    former, latter = latent[:, KV : KV + ROPE // 2], latent[:, KV + ROPE // 2 :]
    key_f = jnp.tile((former * cosine - latter * sine_part).astype(BF), (1, heads))
    key_s = jnp.tile((latter * cosine + former * sine_part).astype(BF), (1, heads))
    expanded = dot_nn(compressed, weight_expand).astype(BF)
    mixed = attend(query_nope, query_f, query_s, expanded, key_f, key_s, length)
    mixed = gather_plane(mixed, 2).reshape(4, 4 * tok_count, nope_cols)
    part = jnp.einsum("ptk,pkn->tn", mixed, weight_output, preferred_element_type=F32)
    part = swap_plane(part.astype(BF).reshape(2, 2, tok_count, out_cols), 3)
    first_sum = tokens + columns_of(part.reshape(4, tok_count, out_cols)).astype(F32)

    normed_two, factor_two = normalize(first_sum)
    hidden_two = (normed_two * ffn_gain).astype(BF)
    h2 = gather_all(hidden_two, nz, 4).reshape(devices * tok_count, width)
    out_part, back_part, grad_in, grad_down, grad_cat, grad_so = ffn(
        h2,
        all_grads,
        slots,
        expert_in,
        expert_down,
        weight_shared,
        own_shared_out,
        hidden,
        capacity,
        units,
        experts,
    )
    spread = (2, 2, nz, 2, tok_count, width)
    grad_h2 = sum_all(back_part.reshape(spread), nz, 5)
    ffn_out = sum_all(out_part.reshape(spread), nz, 6)
    output = (first_sum + ffn_out).astype(BF)[None]
    grad_out = cotangent[0].astype(F32)
    grad_norm, grad_ffn = norm_back(grad_h2, normed_two, factor_two, ffn_gain)
    grad_first = grad_out + grad_norm

    low = jnp.moveaxis(grad_first.astype(BF).reshape(tok_count, 4, out_cols), 1, 0)
    low = swap_plane(low.reshape(2, 2, tok_count, out_cols), 7).reshape(-1, out_cols)
    grad_mixed = jnp.einsum("tn,pkn->ptk", low, weight_output, preferred_element_type=F32)
    grad_mixed = sum_plane(grad_mixed.astype(BF).reshape(2, 2, 4 * tok_count, nope_cols), 8)
    grad_wo = jnp.einsum("ptk,tn->pkn", mixed, low, preferred_element_type=F32)
    gqn, gqf, gqs, gex, gkf, gks = attend_back(
        query_nope, query_f, query_s, expanded, key_f, key_s, grad_mixed.astype(BF), length
    )
    grad_comp = dot_nt(gex, weight_expand)
    grad_we = dot_tn(compressed, gex)
    lat_cols = KV + ROPE
    lat_pad = -(-lat_cols // LANES) * LANES - lat_cols
    grad_lat = jnp.concatenate(
        [
            grad_comp,
            jnp.sum(gkf.reshape(-1, heads, ROPE // 2), axis=1),
            jnp.sum(gks.reshape(-1, heads, ROPE // 2), axis=1),
            jnp.zeros((4 * tok_count, lat_pad), F32),
        ],
        axis=1,
    ).astype(BF)
    grad_lat = sum_plane(grad_lat.reshape(2, 2, tok_count, -1), 9)

    def own_rows(operand):
        return lax.dynamic_slice_in_dim(operand, place * tok_count, tok_count, axis=0)

    grad_lat_in, grad_lat_gain = norm_back(
        grad_lat[:, :KV], own_rows(normed_lat), own_rows(factor_lat), latent_gain
    )
    own_cos, own_sin = own_rows(cosine), own_rows(sine_part)
    former, latter = grad_lat[:, KV : KV + ROPE // 2], grad_lat[:, KV + ROPE // 2 : lat_cols]
    own_latent = jnp.concatenate(
        [
            grad_lat_in,
            former * own_cos + latter * own_sin,
            latter * own_cos - former * own_sin,
            jnp.zeros((tok_count, lat_pad), F32),
        ],
        axis=1,
    ).astype(BF)
    grad_latent = gather_plane(own_latent, 10).reshape(4 * tok_count, -1)[:, :lat_cols]
    grad_query = jnp.concatenate(
        [
            gqn,
            (gqf * cosines + gqs * sines).astype(BF),
            (gqs * cosines - gqf * sines).astype(BF),
        ],
        axis=1,
    )
    grad_wq = dot_tn(h1, grad_query)
    grad_wl = dot_tn(h1, plane_part(grad_latent, place, 1))
    grad_h1 = dot_nt(grad_query, weight_query).astype(BF)
    grad_h1 = sum_plane(grad_h1.reshape(2, 2, tok_count, width), 11)
    grad_h1 = grad_h1 + dot_nt(own_latent[:, :lat_cols], weight_latent)
    grad_tokens, grad_attn = norm_back(grad_h1, normed_one, factor_one, attn_gain)
    grad_inputs = (grad_first + grad_tokens).astype(BF)[None]

    grads = jnp.concatenate(
        [grad_wq.astype(BF), grad_wo.reshape(width, out_cols).astype(BF), grad_wl.astype(BF)],
        axis=1,
    )
    grads = lax.psum_scatter(grads, "expert", scatter_dimension=0, tiled=True)
    grads = lax.all_gather(grads, PLANE, axis=0)
    grad_we = lax.psum_scatter(grad_we.astype(BF), "expert", scatter_dimension=0, tiled=True)
    grad_we = lax.all_gather(grad_we, PLANE, axis=1, tiled=True).astype(F32)
    grad_wq = jnp.concatenate(
        [
            grads[:, :, :nope_cols].reshape(4, local_rows, heads, NOPE),
            grads[:, :, nope_cols : nope_cols + rope_cols].reshape(4, local_rows, heads, -1),
            grads[:, :, nope_cols + rope_cols : query_cols].reshape(4, local_rows, heads, -1),
        ],
        axis=3,
    )
    grad_wq = columns_of(grad_wq.reshape(4, local_rows, -1)).astype(F32)
    grad_wo = columns_of(grads[:, :, query_cols : query_cols + out_cols]).astype(F32)
    grad_wl = columns_of(grads[:, :, query_cols + out_cols :]).astype(F32)
    shared_in = jnp.concatenate([grad_cat[:units], grad_cat[LANES : LANES + units]], axis=0)
    shared_in = lax.all_to_all(
        shared_in.astype(BF).reshape(2 * units, groups, local_rows),
        "expert",
        split_axis=1,
        concat_axis=0,
        tiled=True,
    )
    shared_in = lax.all_gather(shared_in.reshape(-1, local_rows), PLANE, axis=0)
    shared_in = shared_in.reshape(4, groups, 2, units, local_rows)
    shared_in = shared_in.transpose(4, 2, 1, 0, 3).reshape(local_rows, -1).astype(F32)
    shared_out = lax.all_gather(grad_so[:units].astype(BF), PLANE, axis=0, tiled=True).astype(F32)
    small = jnp.concatenate(
        [
            grad_cat[units : units + experts],
            grad_attn[None],
            grad_ffn[None],
            jnp.pad(grad_lat_gain, (0, width - KV))[None],
        ],
        axis=0,
    )
    small = lax.psum(small, ALL)
    rows = plane_part(small, spot, 1, groups)
    lat_rows = plane_part(small[experts + 2, :KV], spot, 0, groups)
    return (
        output,
        grad_inputs,
        rows[experts],
        grad_wq,
        grad_wl,
        lat_rows,
        grad_we,
        grad_wo,
        rows[experts + 1],
        rows[:experts].T,
        shared_in,
        shared_out,
        grad_in,
        grad_down,
    )


def rotate(operand, cosine, sine_part):
    half_width = operand.shape[-1] // 2
    former = operand[..., :half_width]
    latter = operand[..., half_width:]
    return jnp.concatenate(
        [former * cosine - latter * sine_part, latter * cosine + former * sine_part], axis=-1
    )


def across(left_side, right_side):
    return lax.dot_general(
        left_side, right_side, (((0,), (0,)), ((), ())), preferred_element_type=jnp.float32
    )


def against(left_side, right_side):
    return lax.dot_general(
        left_side, right_side, (((1,), (1,)), ((), ())), preferred_element_type=jnp.float32
    )


def to_experts(buffer):
    return lax.all_to_all(buffer, "expert", split_axis=0, concat_axis=2, tiled=True)


def from_experts(buffer):
    return lax.all_to_all(buffer, "expert", split_axis=2, concat_axis=0, tiled=True)


def share_rows(row_block):
    return lax.all_gather(row_block, ("dp", "ctx"), axis=1, tiled=True)


def sum_rows(partial_value):
    return lax.psum_scatter(
        partial_value.astype(jnp.bfloat16), ("dp", "ctx"), scatter_dimension=1, tiled=True
    ).astype(jnp.float32)


def key_scores(query_r, keys_nope, keys_rope, allowed, scale_factor):
    scores = jnp.einsum(
        "qhd,khd->hqk", query_r[..., :NOPE], keys_nope, preferred_element_type=jnp.float32
    )
    scores = scores + jnp.einsum(
        "qhd,kd->hqk", query_r[..., NOPE:], keys_rope, preferred_element_type=jnp.float32
    )
    return jnp.where(allowed[None], scores * scale_factor, -1e30)


def general_body(
    layer_input,
    cotangent,
    routes,
    attn_gain,
    w_query,
    w_latent,
    latent_gain,
    w_expand,
    w_output,
    ffn_gain,
    w_router,
    w_shared_in,
    w_shared_out,
    w_expert_in,
    w_expert_out,
):
    (
        weight_query,
        weight_latent,
        weight_expand,
        weight_output,
        weight_router,
        weight_shared_in,
        weight_shared_out,
    ) = (
        lax.all_gather(w_query, "expert", axis=0, tiled=True),
        lax.all_gather(w_latent, "expert", axis=0, tiled=True),
        lax.all_gather(w_expand, "expert", axis=0, tiled=True),
        lax.all_gather(w_output, "expert", axis=0, tiled=True),
        lax.all_gather(w_router, "expert", axis=0, tiled=True),
        lax.all_gather(w_shared_in, "expert", axis=0, tiled=True),
        lax.all_gather(w_shared_out, "expert", axis=0, tiled=True),
    )
    tokens = layer_input[0].astype(jnp.float32)
    tok_count = tokens.shape[0]
    row_width = tokens.shape[1]
    experts = weight_router.shape[1]
    groups = lax.axis_size("expert")
    local_experts = experts // groups
    capacity = tok_count * TOP * 4 // (3 * experts)
    assigns = tok_count * TOP
    shared_width = weight_shared_out.shape[0]
    places = lax.axis_index("ctx") * tok_count + jnp.arange(tok_count, dtype=jnp.int32)
    inverse = 10000.0 ** (-jnp.arange(0, ROPE, 2).astype(jnp.float32) / ROPE)
    angles = places.astype(jnp.float32)[:, None] * inverse[None, :]
    cosine = jnp.cos(angles)
    sine_part = jnp.sin(angles)
    normed_one, factor_one = normalize(tokens)
    hidden_one = (normed_one * attn_gain).astype(jnp.bfloat16)
    queries = jnp.dot(hidden_one, weight_query, preferred_element_type=jnp.float32).reshape(
        tok_count, HEADS, NOPE + ROPE
    )
    query_r = jnp.concatenate(
        [
            queries[..., :NOPE],
            rotate(queries[..., NOPE:], cosine[:, None, :], sine_part[:, None, :]),
        ],
        axis=-1,
    ).astype(jnp.bfloat16)
    latent = jnp.dot(hidden_one, weight_latent, preferred_element_type=jnp.float32)
    normed_lat, factor_lat = normalize(latent[:, :KV])
    compressed = (normed_lat * latent_gain).astype(jnp.bfloat16)
    key_rope = rotate(latent[:, KV:], cosine, sine_part).astype(jnp.bfloat16)
    packed = jnp.concatenate([compressed, key_rope], axis=1)
    all_keys = lax.all_gather(packed, "ctx", axis=0, tiled=True)
    every_comp = all_keys[:, :KV]
    every_rope = all_keys[:, KV:]
    expanded = (
        jnp.dot(every_comp, weight_expand, preferred_element_type=jnp.float32)
        .astype(jnp.bfloat16)
        .reshape(-1, HEADS, NOPE + VH)
    )
    keys_nope = expanded[..., :NOPE]
    values = expanded[..., NOPE:]
    scale_factor = 1.0 / math.sqrt(NOPE + ROPE)
    allowed = jnp.arange(all_keys.shape[0], dtype=jnp.int32)[None, :] <= places[:, None]
    scores = key_scores(query_r, keys_nope, every_rope, allowed, scale_factor)
    highest = jnp.max(scores, axis=-1, keepdims=True)
    exponent = jnp.exp(scores - highest)
    totals = jnp.sum(exponent, axis=-1, keepdims=True)
    logsum = highest + jnp.log(totals)
    weights = (exponent / totals).astype(jnp.bfloat16)
    mixed_heads = (
        jnp.einsum("hqk,khd->qhd", weights, values, preferred_element_type=jnp.float32)
        .reshape(tok_count, HEADS * VH)
        .astype(jnp.bfloat16)
    )
    first_sum = tokens + jnp.dot(mixed_heads, weight_output, preferred_element_type=jnp.float32)
    normed_two, factor_two = normalize(first_sum)
    hidden_two = (normed_two * ffn_gain).astype(jnp.bfloat16)
    logits = jnp.dot(hidden_two, weight_router, preferred_element_type=jnp.float32)
    router_top = jnp.max(logits, axis=-1, keepdims=True)
    router_exp = jnp.exp(logits - router_top)
    router = router_exp / jnp.sum(router_exp, axis=-1, keepdims=True)
    own_routes = routes[0]
    chosen = own_routes[:, :, None] == jnp.arange(experts, dtype=jnp.int32)[None, None, :]
    picked = jnp.sum(jnp.where(chosen, router[:, None, :], 0.0), axis=2)
    shared_gu = jnp.dot(hidden_two, weight_shared_in, preferred_element_type=jnp.float32)
    shared_gate = shared_gu[:, :shared_width]
    shared_up = shared_gu[:, shared_width:]
    shared_silu, shared_slope = silu_parts(shared_gate)
    shared_act = (shared_silu * shared_up).astype(jnp.bfloat16)
    shared = jnp.dot(shared_act, weight_shared_out, preferred_element_type=jnp.float32)
    picked_ids = own_routes.reshape(-1)
    onehot = (picked_ids[:, None] == jnp.arange(experts, dtype=jnp.int32)[None, :]).astype(
        jnp.int32
    )
    position = jnp.sum((jnp.cumsum(onehot, axis=0) - onehot) * onehot, axis=1)
    target = picked_ids * capacity + position
    holder = (
        jnp.full((experts * capacity,), assigns, jnp.int32)
        .at[target]
        .set(jnp.arange(assigns, dtype=jnp.int32))
    )
    padded = jnp.concatenate([hidden_two, jnp.zeros((1, row_width), jnp.bfloat16)], axis=0)
    outgoing = padded[holder // TOP].reshape(groups, local_experts, capacity, row_width)
    incoming = to_experts(outgoing)[0]
    expert_input = share_rows(incoming)
    paired = jnp.einsum(
        "erd,egfd->ergf", expert_input, w_expert_in, preferred_element_type=jnp.float32
    )
    expert_gate = paired[:, :, 0]
    expert_up = paired[:, :, 1]
    expert_silu, expert_slope = silu_parts(expert_gate)
    expert_act = (expert_silu * expert_up).astype(jnp.bfloat16)
    partial_value = jnp.einsum(
        "erf,efd->erd", expert_act, w_expert_out, preferred_element_type=jnp.float32
    )
    expert_out = sum_rows(partial_value).astype(jnp.bfloat16)
    returned = from_experts(expert_out[None]).reshape(experts * capacity, row_width)
    gathered = returned[target].reshape(tok_count, TOP, row_width).astype(jnp.float32)
    routed = jnp.sum(picked[:, :, None] * gathered, axis=1)
    output = (first_sum + shared + routed).astype(jnp.bfloat16)[None]
    grad_out = cotangent[0].astype(jnp.float32)
    grad_picked = jnp.sum(grad_out[:, None, :] * gathered, axis=2)
    sending = (
        (picked[:, :, None] * grad_out[:, None, :]).astype(jnp.bfloat16).reshape(assigns, row_width)
    )
    sending = jnp.concatenate([sending, jnp.zeros((1, row_width), jnp.bfloat16)], axis=0)[holder]
    grad_expert_out = to_experts(sending.reshape(groups, local_experts, capacity, row_width))[0]
    grad_expert_out = share_rows(grad_expert_out)
    grad_act = jnp.einsum(
        "erd,efd->erf", grad_expert_out, w_expert_out, preferred_element_type=jnp.float32
    )
    grad_weight_out = jnp.einsum(
        "erf,erd->efd", expert_act, grad_expert_out, preferred_element_type=jnp.float32
    )
    grad_paired = jnp.stack(
        [grad_act * expert_up * expert_slope, grad_act * expert_silu], axis=2
    ).astype(jnp.bfloat16)
    grad_weight_in = jnp.einsum(
        "ergf,erd->egfd", grad_paired, expert_input, preferred_element_type=jnp.float32
    )
    grad_input_part = jnp.einsum(
        "ergf,egfd->erd", grad_paired, w_expert_in, preferred_element_type=jnp.float32
    )
    grad_rows_sum = sum_rows(grad_input_part)
    grad_back = from_experts(grad_rows_sum.astype(jnp.bfloat16)[None]).reshape(
        experts * capacity, row_width
    )
    grad_hidden_two = jnp.sum(
        grad_back[target].reshape(tok_count, TOP, row_width).astype(jnp.float32), axis=1
    )
    grad_router = jnp.sum(jnp.where(chosen, grad_picked[:, :, None], 0.0), axis=1)
    grad_logits = (
        router * (grad_router - jnp.sum(router * grad_router, axis=1, keepdims=True))
    ).astype(jnp.bfloat16)
    grad_router_weight = across(hidden_two, grad_logits)
    grad_hidden_two = grad_hidden_two + against(grad_logits, weight_router)
    grad_low = grad_out.astype(jnp.bfloat16)
    grad_shared_out = across(shared_act, grad_low)
    grad_shared_act = against(grad_low, weight_shared_out)
    grad_shared_gu = jnp.concatenate(
        [grad_shared_act * shared_up * shared_slope, grad_shared_act * shared_silu], axis=1
    ).astype(jnp.bfloat16)
    grad_shared_in = across(hidden_two, grad_shared_gu)
    grad_hidden_two = grad_hidden_two + against(grad_shared_gu, weight_shared_in)
    grad_first_norm, grad_ffn = norm_back(grad_hidden_two, normed_two, factor_two, ffn_gain)
    grad_first = grad_out + grad_first_norm
    grad_first_low = grad_first.astype(jnp.bfloat16)
    grad_output_weight = across(mixed_heads, grad_first_low)
    grad_mixed = (
        against(grad_first_low, weight_output).astype(jnp.bfloat16).reshape(tok_count, HEADS, VH)
    )
    prob_rows = jnp.exp(key_scores(query_r, keys_nope, every_rope, allowed, scale_factor) - logsum)
    grad_weights = jnp.einsum(
        "qhd,khd->hqk", grad_mixed, values, preferred_element_type=jnp.float32
    )
    grad_scores = (
        prob_rows * (grad_weights - jnp.sum(prob_rows * grad_weights, axis=-1, keepdims=True))
    ).astype(jnp.bfloat16)
    grad_query_nope = (
        jnp.einsum("hqk,khd->qhd", grad_scores, keys_nope, preferred_element_type=jnp.float32)
        * scale_factor
    )
    grad_query_rope = (
        jnp.einsum("hqk,kd->qhd", grad_scores, every_rope, preferred_element_type=jnp.float32)
        * scale_factor
    )
    grad_keys_nope = (
        jnp.einsum(
            "hqk,qhd->khd", grad_scores, query_r[..., :NOPE], preferred_element_type=jnp.float32
        )
        * scale_factor
    )
    grad_keys_rope = (
        jnp.einsum(
            "hqk,qhd->kd", grad_scores, query_r[..., NOPE:], preferred_element_type=jnp.float32
        )
        * scale_factor
    )
    grad_values = jnp.einsum(
        "hqk,qhd->khd", weights, grad_mixed, preferred_element_type=jnp.float32
    )
    grad_expanded = (
        jnp.concatenate([grad_keys_nope, grad_values], axis=-1)
        .reshape(all_keys.shape[0], -1)
        .astype(jnp.bfloat16)
    )
    grad_expand_weight = across(every_comp, grad_expanded)
    grad_every_comp = against(grad_expanded, weight_expand)
    grad_comp, grad_rope_key = (
        lax.psum_scatter(
            grad_every_comp.astype(jnp.bfloat16), "ctx", scatter_dimension=0, tiled=True
        ).astype(jnp.float32),
        lax.psum_scatter(
            grad_keys_rope.astype(jnp.bfloat16), "ctx", scatter_dimension=0, tiled=True
        ).astype(jnp.float32),
    )
    grad_lat_comp, grad_lat_gain = norm_back(grad_comp, normed_lat, factor_lat, latent_gain)
    grad_latent = jnp.concatenate(
        [grad_lat_comp, rotate(grad_rope_key, cosine, -sine_part)], axis=1
    ).astype(jnp.bfloat16)
    grad_query = (
        jnp.concatenate(
            [grad_query_nope, rotate(grad_query_rope, cosine[:, None, :], -sine_part[:, None, :])],
            axis=-1,
        )
        .reshape(tok_count, -1)
        .astype(jnp.bfloat16)
    )
    grad_query_weight = across(hidden_one, grad_query)
    grad_latent_weight = across(hidden_one, grad_latent)
    grad_hidden_one = against(grad_query, weight_query) + against(grad_latent, weight_latent)
    grad_tokens, grad_attn = norm_back(grad_hidden_one, normed_one, factor_one, attn_gain)
    grad_inputs = (grad_first + grad_tokens).astype(jnp.bfloat16)[None]
    sliced = (
        lax.psum_scatter(
            grad_query_weight.astype(jnp.bfloat16), "expert", scatter_dimension=0, tiled=True
        ).astype(jnp.float32),
        lax.psum_scatter(
            grad_latent_weight.astype(jnp.bfloat16), "expert", scatter_dimension=0, tiled=True
        ).astype(jnp.float32),
        lax.psum_scatter(
            grad_expand_weight.astype(jnp.bfloat16), "expert", scatter_dimension=0, tiled=True
        ).astype(jnp.float32),
        lax.psum_scatter(
            grad_output_weight.astype(jnp.bfloat16), "expert", scatter_dimension=0, tiled=True
        ).astype(jnp.float32),
        lax.psum_scatter(
            grad_router_weight.astype(jnp.bfloat16), "expert", scatter_dimension=0, tiled=True
        ).astype(jnp.float32),
        lax.psum_scatter(
            grad_shared_in.astype(jnp.bfloat16), "expert", scatter_dimension=0, tiled=True
        ).astype(jnp.float32),
        lax.psum_scatter(
            grad_shared_out.astype(jnp.bfloat16), "expert", scatter_dimension=0, tiled=True
        ).astype(jnp.float32),
        lax.psum_scatter(
            grad_attn.astype(jnp.bfloat16), "expert", scatter_dimension=0, tiled=True
        ).astype(jnp.float32),
        lax.psum_scatter(
            grad_lat_gain.astype(jnp.bfloat16), "expert", scatter_dimension=0, tiled=True
        ).astype(jnp.float32),
        lax.psum_scatter(
            grad_ffn.astype(jnp.bfloat16), "expert", scatter_dimension=0, tiled=True
        ).astype(jnp.float32),
    )
    summed = (
        lax.psum(sliced[0].astype(jnp.bfloat16), ("dp", "ctx")).astype(jnp.float32),
        lax.psum(sliced[1].astype(jnp.bfloat16), ("dp", "ctx")).astype(jnp.float32),
        lax.psum(sliced[2].astype(jnp.bfloat16), ("dp", "ctx")).astype(jnp.float32),
        lax.psum(sliced[3].astype(jnp.bfloat16), ("dp", "ctx")).astype(jnp.float32),
        lax.psum(sliced[4].astype(jnp.bfloat16), ("dp", "ctx")).astype(jnp.float32),
        lax.psum(sliced[5].astype(jnp.bfloat16), ("dp", "ctx")).astype(jnp.float32),
        lax.psum(sliced[6].astype(jnp.bfloat16), ("dp", "ctx")).astype(jnp.float32),
        lax.psum(sliced[7].astype(jnp.bfloat16), ("dp", "ctx")).astype(jnp.float32),
        lax.psum(sliced[8].astype(jnp.bfloat16), ("dp", "ctx")).astype(jnp.float32),
        lax.psum(sliced[9].astype(jnp.bfloat16), ("dp", "ctx")).astype(jnp.float32),
    )
    return (
        output,
        grad_inputs,
        summed[7],
        summed[0],
        summed[1],
        summed[8],
        summed[2],
        summed[3],
        summed[9],
        summed[4],
        summed[5],
        summed[6],
        grad_weight_in,
        grad_weight_out,
    )


def solution(mesh):
    dense = mesh.shape["dp"] == 2 and mesh.shape["ctx"] == 2 and mesh.shape["expert"] == 8
    return jax.shard_map(
        split_body if dense else general_body,
        mesh=mesh,
        in_specs=(
            P(("dp", "expert"), "ctx", None),
            P(("dp", "expert"), "ctx", None),
            P(("dp", "expert"), "ctx", None),
            P(),
            P("expert", None),
            P("expert", None),
            P(),
            P("expert", None),
            P("expert", None),
            P(),
            P("expert", None),
            P("expert", None),
            P("expert", None),
            P("expert", None, ("dp", "ctx"), None),
            P("expert", ("dp", "ctx"), None),
        ),
        out_specs=(
            P(("dp", "expert"), "ctx", None),
            P(("dp", "expert"), "ctx", None),
            P("expert"),
            P("expert", None),
            P("expert", None),
            P("expert"),
            P("expert", None),
            P("expert", None),
            P("expert"),
            P("expert", None),
            P("expert", None),
            P("expert", None),
            P("expert", None, ("dp", "ctx"), None),
            P("expert", ("dp", "ctx"), None),
        ),
        check_vma=False,
    )
```

```python
import functools
import math

import jax
import jax.numpy as jnp
from jax import lax
from jax.experimental import pallas as pl
from jax.experimental.pallas import tpu as pltpu
from jax.sharding import PartitionSpec as P

HEADS = 16
NOPE = 128
ROPE = 64
VH = 128
KV = 512
TOP = 6


EPS = 1e-06

MESH = pl.DeviceIdType.MESH
ALL = ("dp", "ctx", "expert")
PLANE = ("dp", "ctx")
BF = jnp.bfloat16
F32 = jnp.float32
LANES = 128
CHUNK = 512
VMEM_LIMIT = 66_000_000


def lasting(microseconds):
    return pl.CostEstimate(
        flops=0, transcendentals=0, bytes_accessed=int(microseconds * 3_000_000)
    )


def here():
    spot = lax.axis_index("expert")
    return lax.axis_index("dp"), lax.axis_index("ctx"), spot // 2, lax.rem(spot, 2)


def greet(peers):
    barrier = pltpu.get_barrier_semaphore()
    for peer in peers:
        pl.semaphore_signal(barrier, inc=1, device_id=peer, device_id_type=MESH)
    pl.semaphore_wait(barrier, len(peers))


class Sends:
    def __init__(self, sems):
        self.sems, self.started = sems, []

    def go(self, src, dst, arrival, peer):
        copy = pltpu.make_async_remote_copy(
            src_ref=src,
            dst_ref=dst,
            send_sem=self.sems.at[len(self.started)],
            recv_sem=arrival,
            device_id=peer,
            device_id_type=MESH,
        )
        copy.start()
        self.started.append(copy)

    def drain(self):
        for copy in self.started:
            copy.wait_send()


def arrive(ref, sem, peer):
    pltpu.make_async_remote_copy(
        src_ref=ref, dst_ref=ref, send_sem=sem, recv_sem=sem, device_id=peer, device_id_type=MESH
    ).wait_recv()


def gather_all_kernel(nz, rows, own, out, lsem, ssem, zsem, xsem, ysem, dasem, dbsem, csem):
    x, y, z, c = here()
    half = rows // 2
    first, second = pl.ds(0, half), pl.ds(half, half)
    xn, yn, cn = (1 - x, y, 2 * z + c), (x, 1 - y, 2 * z + c), (x, y, 2 * z + 1 - c)
    source = [lax.rem(z + nz - k, nz) for k in range(nz)]
    zpeers = [(x, y, 2 * lax.rem(z + k, nz) + c) for k in range(1, nz)]
    greet(zpeers + [xn, yn, cn])
    sends = Sends(ssem)
    mine = out.at[x, y, z, c]
    for k in range(1, nz):
        sends.go(own, mine, zsem.at[k], zpeers[k - 1])
    local = pltpu.make_async_copy(own, mine, lsem)
    local.start()

    def column(j, src):
        dst = out.at[x, y, source[j], c]
        sends.go(src, dst, xsem.at[j], xn)
        sends.go(src, dst, ysem.at[j], yn)
        sends.go(src, dst, csem.at[j], cn)

    def sides(j):
        part = out.at[1 - x, y, source[j], c]
        arrive(part, xsem.at[j], xn)
        sends.go(part.at[first], part.at[first], dasem.at[j], yn)
        sends.go(part, part, csem.at[nz + j], cn)
        part = out.at[x, 1 - y, source[j], c]
        arrive(part, ysem.at[j], yn)
        sends.go(part.at[second], part.at[second], dbsem.at[j], xn)
        sends.go(part, part, csem.at[2 * nz + j], cn)

    def corner(j):
        part = out.at[1 - x, 1 - y, source[j], c]
        arrive(part.at[first], dasem.at[j], yn)
        arrive(part.at[second], dbsem.at[j], xn)
        sends.go(part, part, csem.at[3 * nz + j], cn)

    column(0, own)
    for step in range(1, nz + 2):
        if step < nz:
            part = out.at[x, y, source[step], c]
            arrive(part, zsem.at[step], zpeers[0])
            column(step, part)
        if step - 1 < nz:
            sides(step - 1)
        if 0 <= step - 2 < nz:
            corner(step - 2)
    for q, (qx, qy) in enumerate(((x, y), (1 - x, y), (x, 1 - y), (1 - x, 1 - y))):
        for j in range(nz):
            arrive(out.at[qx, qy, source[j], 1 - c], csem.at[q * nz + j], cn)
    sends.drain()
    local.wait()


def gather_all(own, nz, number):
    rows, width = own.shape
    dma = pltpu.SemaphoreType.DMA
    return pl.pallas_call(
        functools.partial(gather_all_kernel, nz, rows),
        out_shape=jax.ShapeDtypeStruct((2, 2, nz, 2, rows, width), own.dtype),
        in_specs=[pl.BlockSpec(memory_space=pltpu.VMEM)],
        out_specs=pl.BlockSpec(memory_space=pl.ANY),
        scratch_shapes=[
            dma(()),
            dma((9 * nz - 1,)),
            dma((nz,)),
            dma((nz,)),
            dma((nz,)),
            dma((nz,)),
            dma((nz,)),
            dma((4 * nz,)),
        ],
        compiler_params=pltpu.CompilerParams(collective_id=number, has_side_effects=True),
        cost_estimate=lasting(86),
        name=f"gather_all_{number}",
    )(own)


def sum_all_kernel(
    nz, rows, part, out, own, rc, rda, rdb, rx, ry, rz, lsem, ssem, csem, dasem, dbsem, xsem, ysem, zsem
):
    x, y, z, c = here()
    half = rows // 2
    first, second = pl.ds(0, half), pl.ds(half, half)
    xn, yn, cn = (1 - x, y, 2 * z + c), (x, 1 - y, 2 * z + c), (x, y, 2 * z + 1 - c)
    dest = [lax.rem(z + 1 + i, nz) for i in range(nz)]
    zpeers = [(x, y, 2 * dest[i] + c) for i in range(nz - 1)]
    greet(zpeers + [xn, yn, cn])
    sends = Sends(ssem)
    quads = ((1 - x, 1 - y), (1 - x, y), (x, 1 - y), (x, y))
    loads = {}
    for i in range(nz):
        for q, (qx, qy) in enumerate(quads):
            sends.go(part.at[qx, qy, dest[i], 1 - c], rc.at[q, i], csem.at[q * nz + i], cn)
            loads[q, i] = pltpu.make_async_copy(
                part.at[qx, qy, dest[i], c], own.at[q, i], lsem.at[q * nz + i]
            )
            loads[q, i].start()

    def base(q, i):
        loads[q, i].wait()
        arrive(rc.at[q, i], csem.at[q * nz + i], cn)

    def val(ref):
        return ref[...].astype(F32)

    def corner(i):
        base(0, i)
        own[0, i] = (val(own.at[0, i]) + val(rc.at[0, i])).astype(BF)
        sends.go(own.at[0, i, first], rda.at[i], dasem.at[i], yn)
        sends.go(own.at[0, i, second], rdb.at[i], dbsem.at[i], xn)

    def sides(i):
        base(1, i)
        own[1, i, second] = (val(own.at[1, i, second]) + val(rc.at[1, i, second])).astype(BF)
        arrive(rda.at[i], dasem.at[i], yn)
        own[1, i, first] = (
            val(own.at[1, i, first]) + val(rc.at[1, i, first]) + val(rda.at[i])
        ).astype(BF)
        sends.go(own.at[1, i], rx.at[i], xsem.at[i], xn)
        base(2, i)
        own[2, i, first] = (val(own.at[2, i, first]) + val(rc.at[2, i, first])).astype(BF)
        arrive(rdb.at[i], dbsem.at[i], xn)
        own[2, i, second] = (
            val(own.at[2, i, second]) + val(rc.at[2, i, second]) + val(rdb.at[i])
        ).astype(BF)
        sends.go(own.at[2, i], ry.at[i], ysem.at[i], yn)

    def column(i):
        base(3, i)
        arrive(rx.at[i], xsem.at[i], xn)
        arrive(ry.at[i], ysem.at[i], yn)
        total = val(own.at[3, i]) + val(rc.at[3, i]) + val(rx.at[i]) + val(ry.at[i])
        if i < nz - 1:
            own[3, i] = total.astype(BF)
            sends.go(own.at[3, i], rz.at[i], zsem.at[i], zpeers[i])
        else:
            for k in range(nz - 1):
                arrive(rz.at[k], zsem.at[k], zpeers[0])
                total = total + val(rz.at[k])
            out[...] = total

    for step in range(nz + 2):
        if step < nz:
            corner(step)
        if 0 <= step - 1 < nz:
            sides(step - 1)
        if 0 <= step - 2 < nz:
            column(step - 2)
    sends.drain()


def sum_all(part, nz, number):
    rows, width = part.shape[-2:]
    dma = pltpu.SemaphoreType.DMA

    def space(*dims):
        return pltpu.VMEM(dims + (width,), BF)

    return pl.pallas_call(
        functools.partial(sum_all_kernel, nz, rows),
        out_shape=jax.ShapeDtypeStruct((rows, width), F32),
        in_specs=[pl.BlockSpec(memory_space=pl.ANY)],
        out_specs=pl.BlockSpec(memory_space=pltpu.VMEM),
        scratch_shapes=[
            space(4, nz, rows),
            space(4, nz, rows),
            space(nz, rows // 2),
            space(nz, rows // 2),
            space(nz, rows),
            space(nz, rows),
            space(nz - 1, rows),
            dma((4 * nz,)),
            dma((9 * nz - 1,)),
            dma((4 * nz,)),
            dma((nz,)),
            dma((nz,)),
            dma((nz,)),
            dma((nz,)),
            dma((nz - 1,)),
        ],
        compiler_params=pltpu.CompilerParams(
            collective_id=number, has_side_effects=True, vmem_limit_bytes=VMEM_LIMIT
        ),
        cost_estimate=lasting(90),
        name=f"sum_all_{number}",
    )(part)


def gather_plane_kernel(rows, own, out, lsem, ssem, rsem):
    x, y, z, c = here()
    half = rows // 2
    first, second = pl.ds(0, half), pl.ds(half, half)
    xn, yn = (1 - x, y, 2 * z + c), (x, 1 - y, 2 * z + c)
    greet([xn, yn])
    sends = Sends(ssem)
    mine = out.at[x, y]
    sends.go(own, mine, rsem.at[0], xn)
    sends.go(own, mine, rsem.at[1], yn)
    local = pltpu.make_async_copy(own, mine, lsem)
    local.start()
    part = out.at[1 - x, y]
    arrive(part, rsem.at[0], xn)
    sends.go(part.at[first], part.at[first], rsem.at[2], yn)
    part = out.at[x, 1 - y]
    arrive(part, rsem.at[1], yn)
    sends.go(part.at[second], part.at[second], rsem.at[3], xn)
    part = out.at[1 - x, 1 - y]
    arrive(part.at[first], rsem.at[2], yn)
    arrive(part.at[second], rsem.at[3], xn)
    sends.drain()
    local.wait()


def gather_plane(own, number):
    rows, width = own.shape
    dma = pltpu.SemaphoreType.DMA
    return pl.pallas_call(
        functools.partial(gather_plane_kernel, rows),
        out_shape=jax.ShapeDtypeStruct((2, 2, rows, width), own.dtype),
        in_specs=[pl.BlockSpec(memory_space=pltpu.VMEM)],
        out_specs=pl.BlockSpec(memory_space=pltpu.VMEM),
        scratch_shapes=[dma(()), dma((4,)), dma((4,))],
        compiler_params=pltpu.CompilerParams(collective_id=number, has_side_effects=True),
        cost_estimate=lasting(22),
        name=f"gather_plane_{number}",
    )(own)


def swap_plane_kernel(part, out, lsem, ssem, rsem):
    x, y, z, c = here()
    spots = ((1 - x, y), (x, 1 - y), (1 - x, 1 - y))
    peers = [(px, py, 2 * z + c) for px, py in spots]
    greet(peers)
    sends = Sends(ssem)
    for k, (px, py) in enumerate(spots):
        sends.go(part.at[px, py], out.at[x, y], rsem.at[k], peers[k])
    local = pltpu.make_async_copy(part.at[x, y], out.at[x, y], lsem)
    local.start()
    for k, (px, py) in enumerate(spots):
        arrive(out.at[px, py], rsem.at[k], peers[k])
    sends.drain()
    local.wait()


def swap_plane(part, number):
    dma = pltpu.SemaphoreType.DMA
    return pl.pallas_call(
        swap_plane_kernel,
        out_shape=jax.ShapeDtypeStruct(part.shape, part.dtype),
        in_specs=[pl.BlockSpec(memory_space=pltpu.VMEM)],
        out_specs=pl.BlockSpec(memory_space=pltpu.VMEM),
        scratch_shapes=[dma(()), dma((3,)), dma((3,))],
        compiler_params=pltpu.CompilerParams(collective_id=number, has_side_effects=True),
        cost_estimate=lasting(12),
        name=f"swap_plane_{number}",
    )(part)


def sum_plane_kernel(rows, part, out, rda, rdb, rx, ry, sx, sy, ssem, rsem):
    x, y, z, c = here()
    half = rows // 2
    first, second = pl.ds(0, half), pl.ds(half, half)
    xn, yn = (1 - x, y, 2 * z + c), (x, 1 - y, 2 * z + c)
    greet([xn, yn])
    sends = Sends(ssem)
    corner, xside, yside = part.at[1 - x, 1 - y], part.at[1 - x, y], part.at[x, 1 - y]
    sends.go(corner.at[first], rda, rsem.at[0], yn)
    sends.go(corner.at[second], rdb, rsem.at[1], xn)
    sends.go(xside.at[second], rx.at[second], rsem.at[2], xn)
    sends.go(yside.at[first], ry.at[first], rsem.at[3], yn)
    arrive(rda, rsem.at[0], yn)
    sx[...] = (xside[first].astype(F32) + rda[...].astype(F32)).astype(BF)
    sends.go(sx, rx.at[first], rsem.at[4], xn)
    arrive(rdb, rsem.at[1], xn)
    sy[...] = (yside[second].astype(F32) + rdb[...].astype(F32)).astype(BF)
    sends.go(sy, ry.at[second], rsem.at[5], yn)
    arrive(rx.at[second], rsem.at[2], xn)
    arrive(ry.at[first], rsem.at[3], yn)
    arrive(rx.at[first], rsem.at[4], xn)
    arrive(ry.at[second], rsem.at[5], yn)
    out[...] = part[x, y].astype(F32) + rx[...].astype(F32) + ry[...].astype(F32)
    sends.drain()


def sum_plane(part, number):
    rows, width = part.shape[-2:]
    dma = pltpu.SemaphoreType.DMA

    def space(count):
        return pltpu.VMEM((count, width), BF)

    return pl.pallas_call(
        functools.partial(sum_plane_kernel, rows),
        out_shape=jax.ShapeDtypeStruct((rows, width), F32),
        in_specs=[pl.BlockSpec(memory_space=pltpu.VMEM)],
        out_specs=pl.BlockSpec(memory_space=pltpu.VMEM),
        scratch_shapes=[
            space(rows // 2),
            space(rows // 2),
            space(rows),
            space(rows),
            space(rows // 2),
            space(rows // 2),
            dma((6,)),
            dma((6,)),
        ],
        compiler_params=pltpu.CompilerParams(collective_id=number, has_side_effects=True),
        cost_estimate=lasting(20),
        name=f"sum_plane_{number}",
    )(part)


def swap_expert_kernel(groups, part, out, lsem, ssem, rsem):
    x, y, z, c = here()
    spot = 2 * z + c
    others = [lax.rem(spot + k, groups) for k in range(1, groups)]
    froms = [lax.rem(spot + groups - k, groups) for k in range(1, groups)]
    greet([(x, y, other) for other in others])
    sends = Sends(ssem)
    for k, other in enumerate(others):
        sends.go(part.at[other], out.at[spot], rsem.at[k], (x, y, other))
    local = pltpu.make_async_copy(part.at[spot], out.at[spot], lsem)
    local.start()
    for k, source in enumerate(froms):
        arrive(out.at[source], rsem.at[k], (x, y, source))
    sends.drain()
    local.wait()


def swap_expert(part, number):
    groups = part.shape[0]
    dma = pltpu.SemaphoreType.DMA
    return pl.pallas_call(
        functools.partial(swap_expert_kernel, groups),
        out_shape=jax.ShapeDtypeStruct(part.shape, part.dtype),
        in_specs=[pl.BlockSpec(memory_space=pltpu.VMEM)],
        out_specs=pl.BlockSpec(memory_space=pltpu.VMEM),
        scratch_shapes=[dma(()), dma((groups - 1,)), dma((groups - 1,))],
        compiler_params=pltpu.CompilerParams(collective_id=number, has_side_effects=True),
        cost_estimate=lasting(20),
        name=f"swap_expert_{number}",
    )(part)


def finish_kernel(nz, rows, part, out, own, rc, rz, lsem, ssem, csem, zsem, psem):
    x, y, z, c = here()
    xn, yn, cn = (1 - x, y, 2 * z + c), (x, 1 - y, 2 * z + c), (x, y, 2 * z + 1 - c)
    dest = [lax.rem(z + 1 + i, nz) for i in range(nz)]
    zpeers = [(x, y, 2 * dest[i] + c) for i in range(nz - 1)]
    greet(zpeers + [xn, yn, cn])
    sends = Sends(ssem)
    half = rows // 2
    spans = (pl.ds(0, half), pl.ds(half, half))
    loads = {}
    for k, span in enumerate(spans):
        for i in range(nz):
            sends.go(part.at[dest[i], 1 - c, span], rc.at[i, span], csem.at[k, i], cn)
            loads[k, i] = pltpu.make_async_copy(
                part.at[dest[i], c, span], own.at[i, span], lsem.at[k, i]
            )
            loads[k, i].start()

    def base(k, i):
        span = spans[k]
        loads[k, i].wait()
        arrive(rc.at[i, span], csem.at[k, i], cn)
        return own[i, span].astype(F32) + rc[i, span].astype(F32)

    for k, span in enumerate(spans):
        for i in range(nz - 1):
            own[i, span] = base(k, i).astype(BF)
            sends.go(own.at[i, span], rz.at[i, span], zsem.at[k, i], zpeers[i])
    for k, span in enumerate(spans):
        total = base(k, nz - 1)
        for i in range(nz - 1):
            arrive(rz.at[i, span], zsem.at[k, i], zpeers[0])
            total = total + rz[i, span].astype(F32)
        out[x, y, span] = total.astype(BF)
        mine = out.at[x, y, span]
        sends.go(mine, mine, psem.at[0, k], xn)
        sends.go(mine, mine, psem.at[1, k], yn)
    side = out.at[1 - x, y]
    arrive(side.at[spans[0]], psem.at[0, 0], xn)
    sends.go(side.at[spans[0]], side.at[spans[0]], psem.at[2, 0], yn)
    arrive(side.at[spans[1]], psem.at[0, 1], xn)
    side = out.at[x, 1 - y]
    arrive(side.at[spans[0]], psem.at[1, 0], yn)
    arrive(side.at[spans[1]], psem.at[1, 1], yn)
    sends.go(side.at[spans[1]], side.at[spans[1]], psem.at[2, 1], xn)
    corner = out.at[1 - x, 1 - y]
    arrive(corner.at[spans[0]], psem.at[2, 0], yn)
    arrive(corner.at[spans[1]], psem.at[2, 1], xn)
    sends.drain()


def finish(part, nz, number):
    rows, width = part.shape[-2:]
    dma = pltpu.SemaphoreType.DMA
    return pl.pallas_call(
        functools.partial(finish_kernel, nz, rows),
        out_shape=jax.ShapeDtypeStruct((2, 2, rows, width), BF),
        in_specs=[pl.BlockSpec(memory_space=pl.ANY)],
        out_specs=pl.BlockSpec(memory_space=pltpu.VMEM),
        scratch_shapes=[
            pltpu.VMEM((nz, rows, width), BF),
            pltpu.VMEM((nz, rows, width), BF),
            pltpu.VMEM((nz - 1, rows, width), BF),
            dma((2, nz)),
            dma((4 * nz + 4,)),
            dma((2, nz)),
            dma((2, nz - 1)),
            dma((3, 2)),
        ],
        compiler_params=pltpu.CompilerParams(
            collective_id=number, has_side_effects=True, vmem_limit_bytes=VMEM_LIMIT
        ),
        cost_estimate=lasting(70),
        name=f"finish_{number}",
    )(part)


def dot_nn(left, right):
    return lax.dot_general(left, right, (((1,), (0,)), ((), ())), preferred_element_type=F32)


def dot_nt(left, right):
    return lax.dot_general(left, right, (((1,), (1,)), ((), ())), preferred_element_type=F32)


def dot_tn(left, right):
    return lax.dot_general(left, right, (((0,), (0,)), ((), ())), preferred_element_type=F32)


def silu_parts(operand):
    sigmoid_of = jax.nn.sigmoid(operand)
    return (operand * sigmoid_of, sigmoid_of * (1.0 + operand * (1.0 - sigmoid_of)))


def ffn_kernel(
    dims,
    h_all,
    g_all,
    pos,
    win,
    wout,
    wcat,
    wso,
    o_out,
    o_gh,
    o_gwin,
    o_gwout,
    o_gwcat,
    o_gwso,
    o_swap,
    mine,
    rc,
    rd,
    rx,
    ry,
    rz,
    hb,
    gb,
    ob,
    rows,
    grows,
    gwin,
    gwout,
    gwcat,
    gwso,
    stin,
    stout,
    swap,
    l_h,
    l_g,
    l_own,
    l_in,
    l_out,
    l_end,
    s_rc,
    s_d,
    s_x,
    s_y,
    s_z,
    s_swap,
    a_rc,
    a_d,
    a_x,
    a_y,
    a_z,
    a_swap,
):
    nz, tok, hidden, padded, slots, shared, experts = dims
    groups = 2 * nz
    width = h_all.shape[1]
    block = 2 * tok
    per = 2 * slots
    half = tok // 2
    steps = 2 * nz
    x, y, z, c = here()
    spot = 2 * z + c
    xn, yn, cn = (1 - x, y, spot), (x, 1 - y, spot), (x, y, 2 * z + 1 - c)
    others = [lax.rem(spot + k, groups) for k in range(1, groups)]
    froms = [lax.rem(spot + groups - k, groups) for k in range(1, groups)]
    greet([xn, yn] + [(x, y, other) for other in others])
    first, second = pl.ds(0, half), pl.ds(half, half)

    def dest(i):
        return lax.rem(z + 1 + i, nz)

    def zpeer(i):
        return (x, y, 2 * dest(i) + c)

    def unit_start(s, u):
        qx = jnp.where(lax.rem(s, 2) == 0, 1 - x, x)
        qy = y if u else 1 - y
        return pl.multiple_of(((qx * 2 + qy) * nz + dest(s // 2)) * block, block)

    def tiles(s, slot):
        for u in range(2):
            at, to = pl.ds(unit_start(s, u), block), pl.ds(u * block, block)
            yield pltpu.make_async_copy(h_all.at[at], hb.at[slot, to], l_h.at[slot, u])
            yield pltpu.make_async_copy(
                g_all.at[at, pl.ds(0, width)], gb.at[slot, to], l_g.at[slot, u]
            )

    def own_writes(s):
        for u in range(2):
            for t in range(2):
                yield pltpu.make_async_copy(
                    ob.at[t, pl.ds(u * block + c * tok, tok)],
                    mine.at[2 * s + u, t],
                    l_own.at[u, t],
                )

    def remote(src, dst, send_sem, arrival, peer):
        return pltpu.make_async_remote_copy(
            src_ref=src,
            dst_ref=dst,
            send_sem=send_sem,
            recv_sem=arrival,
            device_id=peer,
            device_id_type=MESH,
        )

    def core_sends(s):
        for u in range(2):
            for t in range(2):
                yield remote(
                    ob.at[t, pl.ds(u * block + (1 - c) * tok, tok)],
                    rc.at[2 * s + u, t],
                    s_rc.at[u, t],
                    a_rc.at[2 * s + u, t],
                    cn,
                )

    def unit_of(kind, i):
        return 4 * i + "dxyo".index(kind)

    def loads(kind, i, t, p):
        n = unit_of(kind, i)
        yield pltpu.make_async_copy(mine.at[n, t], stin.at[p, 0], l_in.at[p, 0])
        yield pltpu.make_async_copy(rc.at[n, t], stin.at[p, 1], l_in.at[p, 1])
        if kind == "x":
            yield pltpu.make_async_copy(rd.at[i, t, 0], stin.at[p, 2, first], l_in.at[p, 2])
        if kind == "y":
            yield pltpu.make_async_copy(rd.at[i, t, 1], stin.at[p, 2, second], l_in.at[p, 2])
        if kind == "o":
            yield pltpu.make_async_copy(rx.at[i, t], stin.at[p, 2], l_in.at[p, 2])
            yield pltpu.make_async_copy(ry.at[i, t], stin.at[p, 3], l_in.at[p, 3])

    def begin(kind, i, t, p):
        n = unit_of(kind, i)
        arrive(rc.at[n, t], a_rc.at[n, t], cn)
        if kind == "x":
            arrive(rd.at[i, t, 0], a_d.at[i, t, 0], yn)
        if kind == "y":
            arrive(rd.at[i, t, 1], a_d.at[i, t, 1], xn)
        if kind == "o":
            arrive(rx.at[i, t], a_x.at[i, t], xn)
            arrive(ry.at[i, t], a_y.at[i, t], yn)
        for copy in loads(kind, i, t, p):
            copy.start()

    def val(ref):
        return ref[...].astype(F32)

    def write_back(kind, i, t, p):
        return pltpu.make_async_copy(stout.at[p], mine.at[unit_of(kind, i), t], l_out.at[p])

    def settle(kind, i, t, p):
        for copy in loads(kind, i, t, p):
            copy.wait()
        if kind == "d":
            stout[p] = (val(stin.at[p, 0]) + val(stin.at[p, 1])).astype(BF)
        elif kind == "o":
            stout[p] = (
                val(stin.at[p, 0]) + val(stin.at[p, 1]) + val(stin.at[p, 2]) + val(stin.at[p, 3])
            ).astype(BF)
        else:
            more, same = (first, second) if kind == "x" else (second, first)
            stout[p, more] = (
                val(stin.at[p, 0, more]) + val(stin.at[p, 1, more]) + val(stin.at[p, 2, more])
            ).astype(BF)
            stout[p, same] = (val(stin.at[p, 0, same]) + val(stin.at[p, 1, same])).astype(BF)
        write_back(kind, i, t, p).start()

    def outgoing(kind, i, t):
        src = mine.at[unit_of(kind, i), t]
        if kind == "d":
            yield remote(src.at[first], rd.at[i, t, 0], s_d.at[i, t, 0], a_d.at[i, t, 0], yn)
            yield remote(src.at[second], rd.at[i, t, 1], s_d.at[i, t, 1], a_d.at[i, t, 1], xn)
        if kind == "x":
            yield remote(src, rx.at[i, t], s_x.at[i, t], a_x.at[i, t], xn)
        if kind == "y":
            yield remote(src, ry.at[i, t], s_y.at[i, t], a_y.at[i, t], yn)
        if kind == "o":
            yield remote(src, rz.at[i, t], s_z.at[i, t], a_z.at[i, t], zpeer(i))

    def launch(kind, i, t, p):
        write_back(kind, i, t, p).wait()
        for copy in outgoing(kind, i, t):
            copy.start()

    def serve(action, s, k):
        odd = lax.rem(s, 2) == 1
        t, p = k % 2, k % 2
        if k < 2:

            @pl.when(odd & (s >= 3))
            def _():
                action("o", (s - 3) // 2, t, p)

            @pl.when(jnp.logical_not(odd) & (s >= 2))
            def _():
                action("x", (s - 2) // 2, t, p)
        else:

            @pl.when(odd)
            def _():
                action("d", (s - 1) // 2, t, p)

            @pl.when(jnp.logical_not(odd) & (s >= 2))
            def _():
                action("y", (s - 2) // 2, t, p)

    for copy in tiles(0, 0):
        copy.start()
    gwin[...] = jnp.zeros_like(gwin)
    gwout[...] = jnp.zeros_like(gwout)
    gwcat[...] = jnp.zeros_like(gwcat)
    gwso[...] = jnp.zeros_like(gwso)

    def chunks(body):
        def run(n, carry):
            body(pl.ds(pl.multiple_of(n * CHUNK, CHUNK), CHUNK))
            return carry

        lax.fori_loop(0, width // CHUNK, run, 0)

    first_lane = shared + 2 * spot

    def step(s, carry):
        slot = lax.rem(s, 2)
        for copy in tiles(s, slot):
            copy.wait()

        @pl.when(s + 1 < steps)
        def _():
            for copy in tiles(s + 1, 1 - slot):
                copy.start()

        @pl.when(s >= 1)
        def _():
            for copy in own_writes(s - 1):
                copy.wait()

        serve(begin, s, 0)
        mixed = dot_nn(hb[slot], wcat[...])
        gate, up = mixed[:, :LANES], mixed[:, LANES:]
        lane = lax.broadcasted_iota(jnp.int32, gate.shape, 1)
        of_router = (lane >= shared) & (lane < shared + experts)
        logits = jnp.where(of_router, gate, -1e30)
        raised = jnp.where(
            of_router, jnp.exp(logits - jnp.max(logits, axis=1, keepdims=True)), 0.0
        )
        router = raised / jnp.sum(raised, axis=1, keepdims=True)
        silu, slope = silu_parts(gate)
        act = (silu * up).astype(BF)
        gact = dot_nt(gb[slot], wso[...])
        ggate = gact * up * slope
        gup = gact * silu
        high = router.astype(BF)
        router_parts = jnp.concatenate([high, (router - high.astype(F32)).astype(BF)], axis=1)
        serve(settle, s, 0)
        serve(begin, s, 1)
        slot_lane = lax.broadcasted_iota(jnp.int32, (per, LANES), 1)
        slot_row = lax.broadcasted_iota(jnp.int32, (per, block), 0)
        picks, picked = [], [[], []]
        for u in range(2):
            span = slice(u * block, (u + 1) * block)
            place = slice(u * per, (u + 1) * per)
            lanes = pl.ds(unit_start(s, u), block)
            pick = jnp.concatenate(
                [
                    jnp.where(pos[j : j + 1, lanes] == slot_row, 1.0, 0.0).astype(BF)
                    for j in range(2)
                ],
                axis=0,
            )
            picks.append(pick)

            def fetch(cols, pick=pick, span=span, place=place):
                taken = dot_nn(pick, hb[slot, span, cols]).astype(BF)
                rows[0, place, cols] = taken[:per]
                rows[1, place, cols] = taken[per:]
                taken = dot_nn(pick, gb[slot, span, cols]).astype(BF)
                grows[0, place, cols] = taken[:per]
                grows[1, place, cols] = taken[per:]

            chunks(fetch)
            taken = dot_nn(pick, router_parts[span])
            taken = taken[:, :LANES] + taken[:, LANES:]
            for j in range(2):
                picked[j].append(
                    jnp.sum(
                        jnp.where(slot_lane == first_lane + j, taken[j * per : (j + 1) * per], 0.0),
                        axis=1,
                        keepdims=True,
                    )
                )
        serve(settle, s, 1)
        serve(launch, s, 0)
        serve(begin, s, 2)
        grad_picked = []
        for j in range(2):
            share = jnp.concatenate(picked[j], axis=0)
            both = dot_nt(rows[j], win[j])
            egate, eup = both[:, :padded], both[:, padded:]
            raw = dot_nt(grows[j], wout[j])
            esilu, eslope = silu_parts(egate)
            eact = esilu * eup
            grad_picked.append(jnp.sum(eact * raw, axis=1, keepdims=True))
            scaled = (share * eact).astype(BF)
            graw = share * raw
            gboth = jnp.concatenate([graw * eup * eslope, graw * esilu], axis=1).astype(BF)

            def expert(cols, j=j, scaled=scaled, gboth=gboth):
                gin, gout = rows[j, :, cols], grows[j, :, cols]
                gwout[j, :, cols] += dot_tn(scaled[:, :hidden], gout)
                gwin[j, 0, :, cols] += dot_tn(gboth[:, :hidden], gin)
                gwin[j, 1, :, cols] += dot_tn(gboth[:, padded : padded + hidden], gin)
                grows[j, :, cols] = dot_nn(scaled, wout[j, :, cols]).astype(BF)
                rows[j, :, cols] = dot_nn(gboth, win[j, :, cols]).astype(BF)

            chunks(expert)
            serve(settle, s, 2 + j)
            serve(launch, s, 1 + j)
            if j == 0:
                serve(begin, s, 3)

        @pl.when(s >= 1)
        def _():
            for copy in core_sends(s - 1):
                copy.wait_send()

        gparts = []
        for u in range(2):
            span = slice(u * block, (u + 1) * block)
            place = slice(u * per, (u + 1) * per)
            pick = picks[u]
            spread = jnp.concatenate(
                [
                    jnp.where(slot_lane == first_lane + j, grad_picked[j][place], 0.0)
                    for j in range(2)
                ],
                axis=0,
            )
            high = spread.astype(BF)
            low = (spread - high.astype(F32)).astype(BF)
            grouter = dot_tn(pick, jnp.concatenate([high, low], axis=1))
            grouter = grouter[:, :LANES] + grouter[:, LANES:]
            share = router[span]
            glogits = share * (grouter - jnp.sum(share * grouter, axis=1, keepdims=True))
            gpart = jnp.concatenate([ggate[span] + glogits, gup[span]], axis=1).astype(BF)
            gparts.append(gpart)

            def spreads(cols, pick=pick, span=span, place=place, gpart=gpart):
                sent = jnp.concatenate([grows[0, place, cols], grows[1, place, cols]], axis=0)
                ob[0, span, cols] = (dot_tn(pick, sent) + dot_nn(act[span], wso[:, cols])).astype(BF)
                sent = jnp.concatenate([rows[0, place, cols], rows[1, place, cols]], axis=0)
                ob[1, span, cols] = (dot_tn(pick, sent) + dot_nt(gpart, wcat[cols, :])).astype(BF)

            chunks(spreads)
        for copy in core_sends(s):
            copy.start()
        for copy in own_writes(s):
            copy.start()
        serve(launch, s, 3)
        gall = jnp.concatenate(gparts, axis=0)

        def dense(cols):
            gwcat[:, cols] += dot_tn(gall, hb[slot, :, cols])
            gwso[:, cols] += dot_tn(act, gb[slot, :, cols])

        chunks(dense)
        return carry

    lax.fori_loop(0, steps, step, 0)
    last = nz - 1
    for copy in own_writes(steps - 1):
        copy.wait()
    ends = [("x", 0), ("x", 1), ("y", 0), ("y", 1)]
    for kind, t in ends[:2]:
        begin(kind, last, t, t)
    for k, (kind, t) in enumerate(ends):
        settle(kind, last, t, t)
        launch(kind, last, t, t)
        if k < 2:
            begin(*ends[k + 2][:1], last, ends[k + 2][1], t)
    finals = [
        pltpu.make_async_copy(src, dst, l_end.at[k])
        for k, (src, dst) in enumerate(
            ((gwin, o_gwin), (gwout, o_gwout), (gwcat, o_gwcat), (gwso, o_gwso))
        )
    ]
    for copy in finals:
        copy.start()
    for e in range(groups):
        cols = slice(e * (width // groups), (e + 1) * (width // groups))
        swap[e, 0] = gwcat[:shared, cols].astype(BF)
        swap[e, 1] = gwcat[LANES : LANES + shared, cols].astype(BF)
    swaps = [
        remote(swap.at[other], o_swap.at[spot], s_swap.at[k], a_swap.at[k], (x, y, other))
        for k, other in enumerate(others)
    ]
    for copy in swaps:
        copy.start()
    kept = pltpu.make_async_copy(swap.at[spot], o_swap.at[spot], l_end.at[4])
    kept.start()
    late = []
    for t in range(2):
        for i in range(nz - 1):
            arrive(rz.at[i, t], a_z.at[i, t], zpeer(0))
            copy = pltpu.make_async_copy(
                rz.at[i, t], hb.at[t, pl.ds(i * tok, tok)], l_h.at[t, 0] if i == 0 else l_g.at[t, i - 1]
            )
            copy.start()
            late.append(copy)
    for t in range(2):
        begin("o", last, t, t)
    for t, out in enumerate((o_out, o_gh)):
        for copy in loads("o", last, t, t):
            copy.wait()
        for copy in late[t * (nz - 1) : (t + 1) * (nz - 1)]:
            copy.wait()
        total = val(stin.at[t, 0]) + val(stin.at[t, 1]) + val(stin.at[t, 2]) + val(stin.at[t, 3])
        for i in range(nz - 1):
            total = total + val(hb.at[t, pl.ds(i * tok, tok)])
        out[...] = total
    for k, source in enumerate(froms):
        arrive(o_swap.at[source], a_swap.at[k], (x, y, source))
    for copy in swaps + list(core_sends(steps - 1)):
        copy.wait_send()
    for i in range(nz):
        for t in range(2):
            for kind in "dxyo" if i < last else "dxy":
                for copy in outgoing(kind, i, t):
                    copy.wait_send()
    kept.wait()
    for copy in finals:
        copy.wait()


def ffn(h, g, pos, win, wout, wcat, wso, nz, tok, hidden, slots, shared, experts, number):
    width = h.shape[1]
    padded = wout.shape[1]
    left = pl.BlockSpec(memory_space=pl.ANY)
    here_spec = pl.BlockSpec(memory_space=pltpu.VMEM)
    dma = pltpu.SemaphoreType.DMA
    sums = [(2, 2, hidden, width), (2, hidden, width), (2 * LANES, width), (LANES, width)]
    piece = (tok, width)
    moved = [
        (2 * nz, 2, shared, width // (2 * nz)),
        (4 * nz, 2) + piece,
        (4 * nz, 2) + piece,
        (nz, 2, 2, tok // 2, width),
        (nz, 2) + piece,
        (nz, 2) + piece,
        (nz - 1, 2) + piece,
    ]
    slot_rows = 4 * slots
    return pl.pallas_call(
        functools.partial(ffn_kernel, (nz, tok, hidden, padded, slots, shared, experts)),
        out_shape=[jax.ShapeDtypeStruct(piece, F32)] * 2
        + [jax.ShapeDtypeStruct(s, F32) for s in sums]
        + [jax.ShapeDtypeStruct(s, BF) for s in moved],
        in_specs=[left, left] + [here_spec] * 5,
        out_specs=[here_spec] * 2 + [left] * (len(sums) + len(moved)),
        scratch_shapes=[
            pltpu.VMEM((2, 4 * tok, width), BF),
            pltpu.VMEM((2, 4 * tok, width), BF),
            pltpu.VMEM((2, 4 * tok, width), BF),
            pltpu.VMEM((2, slot_rows, width), BF),
            pltpu.VMEM((2, slot_rows, width), BF),
        ]
        + [pltpu.VMEM(s, F32) for s in sums]
        + [
            pltpu.VMEM((2, 4) + piece, BF),
            pltpu.VMEM((2,) + piece, BF),
            pltpu.VMEM(moved[0], BF),
            dma((2, 2)),
            dma((2, 2)),
            dma((2, 2)),
            dma((2, 4)),
            dma((2,)),
            dma((5,)),
            dma((2, 2)),
            dma((nz, 2, 2)),
            dma((nz, 2)),
            dma((nz, 2)),
            dma((nz - 1, 2)),
            dma((2 * nz - 1,)),
            dma((4 * nz, 2)),
            dma((nz, 2, 2)),
            dma((nz, 2)),
            dma((nz, 2)),
            dma((nz - 1, 2)),
            dma((2 * nz - 1,)),
        ],
        compiler_params=pltpu.CompilerParams(
            collective_id=number, has_side_effects=True, vmem_limit_bytes=VMEM_LIMIT
        ),
        cost_estimate=lasting(200),
        name="ffn",
    )(h, g, pos, win, wout, wcat, wso)


def head_parts(qn, qf, qs, ex, kf, ks):
    lane = lax.broadcasted_iota(jnp.int32, qf.shape, 1)
    low = pl.program_id(1) * (ROPE // 2)
    mine = (lane >= low) & (lane < low + ROPE // 2)
    zero = jnp.zeros_like(qf[...])
    left = jnp.concatenate(
        [qn[...], jnp.where(mine, qf[...], zero), jnp.where(mine, qs[...], zero)], axis=1
    )
    right = jnp.concatenate([ex[:, :NOPE], kf[...], ks[...]], axis=1)
    scores = dot_nt(left, right) * (1.0 / math.sqrt(NOPE + ROPE))
    row = lax.broadcasted_iota(jnp.int32, scores.shape, 0)
    col = lax.broadcasted_iota(jnp.int32, scores.shape, 1)
    scores = jnp.where(col <= row, scores, -1e30)
    exponent = jnp.exp(scores - jnp.max(scores, axis=1, keepdims=True))
    probs = exponent / jnp.sum(exponent, axis=1, keepdims=True)
    return left, right, probs, mine


def attend_kernel(qn, qf, qs, ex, kf, ks, mixed):
    probs = head_parts(qn, qf, qs, ex, kf, ks)[2]
    mixed[...] = dot_nn(probs.astype(BF), ex[:, NOPE:]).astype(BF)


def attend_back_kernel(qn, qf, qs, ex, kf, ks, gm, gqn, gqf, gqs, gex, gkf, gks):
    left, right, probs, mine = head_parts(qn, qf, qs, ex, kf, ks)
    scale = 1.0 / math.sqrt(NOPE + ROPE)

    @pl.when(pl.program_id(1) == 0)
    def _():
        for ref in (gqf, gqs, gkf, gks):
            ref[...] = jnp.zeros_like(ref)

    gweights = dot_nt(gm[...], ex[:, NOPE:])
    gscores = probs * (gweights - jnp.sum(probs * gweights, axis=1, keepdims=True))
    gscores = gscores.astype(BF)
    gleft = dot_nn(gscores, right) * scale
    gqn[...] = gleft[:, :NOPE].astype(BF)
    gqf[...] += jnp.where(mine, gleft[:, NOPE : NOPE + LANES], 0.0)
    gqs[...] += jnp.where(mine, gleft[:, NOPE + LANES :], 0.0)
    gright = dot_tn(gscores, left) * scale
    gex[:, :NOPE] = gright[:, :NOPE].astype(BF)
    gkf[...] += gright[:, NOPE : NOPE + LANES]
    gks[...] += gright[:, NOPE + LANES :]
    gex[:, NOPE:] = dot_tn(probs.astype(BF), gm[...]).astype(BF)


def attention_specs(length):
    each = pl.BlockSpec((length, NOPE), lambda b, h: (b, h))
    one = pl.BlockSpec((length, LANES), lambda b, h: (b, 0))
    wide = pl.BlockSpec((length, NOPE + VH), lambda b, h: (b, h))
    return each, one, wide


def attend(qn, qf, qs, ex, kf, ks, length):
    each, one, wide = attention_specs(length)
    return pl.pallas_call(
        attend_kernel,
        grid=(qn.shape[0] // length, qn.shape[1] // NOPE),
        out_shape=jax.ShapeDtypeStruct(qn.shape, BF),
        in_specs=[each, one, one, wide, one, one],
        out_specs=each,
        cost_estimate=lasting(8),
        name="attend",
    )(qn, qf, qs, ex, kf, ks)


def attend_back(qn, qf, qs, ex, kf, ks, gm, length):
    each, one, wide = attention_specs(length)
    return pl.pallas_call(
        attend_back_kernel,
        grid=(qn.shape[0] // length, qn.shape[1] // NOPE),
        out_shape=[
            jax.ShapeDtypeStruct(qn.shape, BF),
            jax.ShapeDtypeStruct(qf.shape, F32),
            jax.ShapeDtypeStruct(qf.shape, F32),
            jax.ShapeDtypeStruct(ex.shape, BF),
            jax.ShapeDtypeStruct(qf.shape, F32),
            jax.ShapeDtypeStruct(qf.shape, F32),
        ],
        in_specs=[each, one, one, wide, one, one, each],
        out_specs=[each, one, one, wide, one, one],
        cost_estimate=lasting(11),
        name="attend_back",
    )(qn, qf, qs, ex, kf, ks, gm)


def normalize(operand):
    factor = lax.rsqrt(jnp.mean(operand * operand, axis=-1, keepdims=True) + EPS)
    return (operand * factor, factor)


def norm_back(grad_out, normed, factor, gain_row):
    inner_sums = grad_out * gain_row
    grad_in = factor * (inner_sums - normed * jnp.mean(inner_sums * normed, axis=-1, keepdims=True))
    return (grad_in, jnp.sum(grad_out * normed, axis=0))


def plane_part(operand, index, axis, parts=4):
    size = operand.shape[axis] // parts
    return lax.dynamic_slice_in_dim(operand, index * size, size, axis=axis)


def columns_of(blocks):
    return jnp.moveaxis(blocks, 0, 1).reshape(blocks.shape[1], -1)


def split_body(
    layer_input,
    cotangent,
    routes,
    attn_gain,
    w_query,
    w_latent,
    latent_gain,
    w_expand,
    w_output,
    ffn_gain,
    w_router,
    w_shared_in,
    w_shared_out,
    w_expert_in,
    w_expert_out,
):
    spot = lax.axis_index("expert")
    place = lax.axis_index("dp") * 2 + lax.axis_index("ctx")
    groups = lax.axis_size("expert")
    nz = groups // 2
    tok_count, width = layer_input.shape[1:]
    length = 2 * tok_count
    devices = 4 * groups
    experts = w_router.shape[1]
    capacity = tok_count * TOP * 4 // (3 * experts)
    local_rows = w_query.shape[0]
    heads = HEADS // 4
    nope_cols, rope_cols = heads * NOPE, heads * ROPE // 2
    query_cols = nope_cols + 2 * rope_cols
    out_cols = width // 4
    hidden = w_expert_out.shape[1]
    padded = -(-hidden // LANES) * LANES
    shared_rows = w_shared_out.shape[0]
    units = shared_rows // 4

    tokens = layer_input[0].astype(F32)
    normed_one, factor_one = normalize(tokens)
    hidden_one = (normed_one * attn_gain).astype(BF)
    h1 = gather_plane(hidden_one, 1).reshape(4 * tok_count, width)
    own_query = plane_part(w_query, place, 1).reshape(local_rows, heads, NOPE + ROPE)
    half = NOPE + ROPE // 2
    attn_pack = jnp.concatenate(
        [
            own_query[:, :, :NOPE].reshape(local_rows, nope_cols),
            own_query[:, :, NOPE:half].reshape(local_rows, rope_cols),
            own_query[:, :, half:].reshape(local_rows, rope_cols),
            plane_part(w_output, place, 1),
            w_latent,
        ],
        axis=1,
    )
    attn_w = lax.all_gather(attn_pack, "expert", axis=0, tiled=True)
    weight_expand = lax.all_gather(plane_part(w_expand, place, 1), "expert", axis=0, tiled=True)
    weight_query = attn_w[:, :query_cols]
    weight_output = attn_w[:, query_cols : query_cols + out_cols].reshape(4, out_cols, out_cols)
    weight_latent = attn_w[:, query_cols + out_cols :]

    lanes = jnp.arange(LANES, dtype=jnp.int32)
    named_here = jnp.any(routes[0][:, :, None] == lanes[None, None, :], axis=1)
    all_grads = lax.all_gather(
        jnp.concatenate([cotangent[0], named_here.astype(BF)], axis=1), ALL, axis=0, tiled=True
    )
    all_named = all_grads[:, width : width + experts].reshape(devices, tok_count, experts)
    offset = (jnp.arange(devices, dtype=jnp.int32) % 2 * capacity)[:, None]
    slots = []
    for j in range(2):
        named = lax.dynamic_index_in_dim(all_named, 2 * spot + j, axis=2, keepdims=False) > 0
        order = jnp.cumsum(named.astype(jnp.int32), axis=1) - 1
        slots.append(jnp.where(named, order + offset, -1).reshape(1, -1))
    slots = jnp.concatenate(slots + [jnp.full((6, slots[0].shape[1]), -1, jnp.int32)], axis=0)
    halves = w_shared_in.reshape(local_rows, 2, groups, 4, units)
    halves = lax.dynamic_index_in_dim(halves, place, axis=3, keepdims=False)
    spare = LANES - units - experts
    shared_pack = jnp.concatenate(
        [
            halves[:, 0],
            jnp.broadcast_to(w_router[:, None, :], (local_rows, groups, experts)),
            jnp.zeros((local_rows, groups, spare), BF),
            halves[:, 1],
            jnp.zeros((local_rows, groups, LANES - units), BF),
        ],
        axis=2,
    )
    weight_shared = lax.all_to_all(
        jnp.moveaxis(shared_pack, 1, 0), "expert", split_axis=0, concat_axis=0, tiled=True
    ).reshape(width, 2 * LANES)
    own_shared_out = jnp.pad(plane_part(w_shared_out, place, 0), ((0, LANES - units), (0, 0)))
    widen = padded - hidden
    expert_in = jnp.pad(w_expert_in, ((0, 0), (0, 0), (0, widen), (0, 0))).reshape(
        2, 2 * padded, width
    )
    expert_down = jnp.pad(w_expert_out, ((0, 0), (0, widen), (0, 0)))

    inverse = 10000.0 ** (-jnp.arange(0, ROPE, 2).astype(F32) / ROPE)
    places = jnp.arange(4 * tok_count, dtype=jnp.int32) % length
    angles = places.astype(F32)[:, None] * inverse[None, :]
    cosine, sine_part = jnp.cos(angles), jnp.sin(angles)
    cosines, sines = jnp.tile(cosine, (1, heads)), jnp.tile(sine_part, (1, heads))
    queries = dot_nn(h1, weight_query)
    query_nope = queries[:, :nope_cols].astype(BF)
    former = queries[:, nope_cols : nope_cols + rope_cols]
    latter = queries[:, nope_cols + rope_cols :]
    query_f = (former * cosines - latter * sines).astype(BF)
    query_s = (latter * cosines + former * sines).astype(BF)
    latent = dot_nn(h1, weight_latent)
    normed_lat, factor_lat = normalize(latent[:, :KV])
    compressed = (normed_lat * latent_gain).astype(BF)
    former, latter = latent[:, KV : KV + ROPE // 2], latent[:, KV + ROPE // 2 :]
    key_f = jnp.tile((former * cosine - latter * sine_part).astype(BF), (1, heads))
    key_s = jnp.tile((latter * cosine + former * sine_part).astype(BF), (1, heads))
    expanded = dot_nn(compressed, weight_expand).astype(BF)
    mixed = attend(query_nope, query_f, query_s, expanded, key_f, key_s, length)
    mixed = gather_plane(mixed, 2).reshape(4, 4 * tok_count, nope_cols)
    part = jnp.einsum("ptk,pkn->tn", mixed, weight_output, preferred_element_type=F32)
    part = swap_plane(part.astype(BF).reshape(2, 2, tok_count, out_cols), 3)
    first_sum = tokens + columns_of(part.reshape(4, tok_count, out_cols)).astype(F32)

    normed_two, factor_two = normalize(first_sum)
    hidden_two = (normed_two * ffn_gain).astype(BF)
    h2 = gather_all(hidden_two, nz, 4).reshape(devices * tok_count, width)
    ffn_out, grad_h2, grad_in, grad_down, grad_cat, grad_so, shared_in = ffn(
        h2,
        all_grads,
        slots,
        expert_in,
        expert_down,
        weight_shared,
        own_shared_out,
        nz,
        tok_count,
        hidden,
        capacity,
        units,
        experts,
        5,
    )[:7]
    shared_in = lax.all_gather(shared_in.reshape(-1, local_rows), PLANE, axis=0)
    shared_in = shared_in.reshape(4, groups, 2, units, local_rows)
    shared_in = shared_in.transpose(4, 2, 1, 0, 3).reshape(local_rows, -1).astype(F32)
    shared_out = lax.all_gather(grad_so[:units].astype(BF), PLANE, axis=0, tiled=True).astype(F32)
    output = (first_sum + ffn_out).astype(BF)[None]
    grad_out = cotangent[0].astype(F32)
    grad_norm, grad_ffn = norm_back(grad_h2, normed_two, factor_two, ffn_gain)
    grad_first = grad_out + grad_norm

    low = jnp.moveaxis(grad_first.astype(BF).reshape(tok_count, 4, out_cols), 1, 0)
    low = swap_plane(low.reshape(2, 2, tok_count, out_cols), 7).reshape(-1, out_cols)
    grad_mixed = jnp.einsum("tn,pkn->ptk", low, weight_output, preferred_element_type=F32)
    grad_mixed = sum_plane(grad_mixed.astype(BF).reshape(2, 2, 4 * tok_count, nope_cols), 8)
    grad_wo = jnp.einsum("ptk,tn->pkn", mixed, low, preferred_element_type=F32)
    early = jnp.concatenate(
        [
            grad_wo.reshape(width, out_cols).astype(BF),
            grad_cat[units : units + experts].T.astype(BF),
            grad_ffn[:, None].astype(BF),
            jnp.zeros((width, LANES - experts - 1), BF),
        ],
        axis=1,
    )
    early = lax.psum_scatter(early, "expert", scatter_dimension=0, tiled=True)
    early = lax.all_gather(early, PLANE, axis=0)
    grad_wo = columns_of(early[:, :, :out_cols]).astype(F32)
    sums = jnp.sum(early[:, :, out_cols : out_cols + experts + 1].astype(F32), axis=0)
    grad_wr, grad_ffn = sums[:, :experts], sums[:, experts]
    gqn, gqf, gqs, gex, gkf, gks = attend_back(
        query_nope, query_f, query_s, expanded, key_f, key_s, grad_mixed.astype(BF), length
    )
    grad_comp = dot_nt(gex, weight_expand)
    lat_cols = KV + ROPE
    lat_pad = -(-lat_cols // LANES) * LANES - lat_cols
    grad_lat = jnp.concatenate(
        [
            grad_comp,
            jnp.sum(gkf.reshape(-1, heads, ROPE // 2), axis=1),
            jnp.sum(gks.reshape(-1, heads, ROPE // 2), axis=1),
            jnp.zeros((4 * tok_count, lat_pad), F32),
        ],
        axis=1,
    ).astype(BF)
    grad_lat = sum_plane(grad_lat.reshape(2, 2, tok_count, -1), 9)

    def own_rows(operand):
        return lax.dynamic_slice_in_dim(operand, place * tok_count, tok_count, axis=0)

    grad_lat_in, grad_lat_gain = norm_back(
        grad_lat[:, :KV], own_rows(normed_lat), own_rows(factor_lat), latent_gain
    )
    grad_we = jnp.concatenate(
        [
            dot_tn(compressed, gex).astype(BF),
            grad_lat_gain[:, None].astype(BF),
            jnp.zeros((KV, LANES - 1), BF),
        ],
        axis=1,
    )
    grad_we = lax.psum_scatter(grad_we, "expert", scatter_dimension=0, tiled=True)
    grad_we = lax.all_gather(grad_we, PLANE, axis=0)
    grad_lat_gain = jnp.sum(grad_we[:, :, heads * (NOPE + VH)].astype(F32), axis=0)
    grad_we = columns_of(grad_we[:, :, : heads * (NOPE + VH)]).astype(F32)
    own_cos, own_sin = own_rows(cosine), own_rows(sine_part)
    former, latter = grad_lat[:, KV : KV + ROPE // 2], grad_lat[:, KV + ROPE // 2 : lat_cols]
    own_latent = jnp.concatenate(
        [
            grad_lat_in,
            former * own_cos + latter * own_sin,
            latter * own_cos - former * own_sin,
            jnp.zeros((tok_count, lat_pad), F32),
        ],
        axis=1,
    ).astype(BF)
    grad_latent = gather_plane(own_latent, 10).reshape(4 * tok_count, -1)[:, :lat_cols]
    grad_query = jnp.concatenate(
        [
            gqn,
            (gqf * cosines + gqs * sines).astype(BF),
            (gqs * cosines - gqf * sines).astype(BF),
        ],
        axis=1,
    )
    grad_wq = dot_tn(h1, grad_query)
    grad_wl = dot_tn(h1, plane_part(grad_latent, place, 1))
    grad_h1 = dot_nt(grad_query, weight_query).astype(BF)
    grad_h1 = sum_plane(grad_h1.reshape(2, 2, tok_count, width), 11)
    grad_h1 = grad_h1 + dot_nt(own_latent[:, :lat_cols], weight_latent)
    grad_tokens, grad_attn = norm_back(grad_h1, normed_one, factor_one, attn_gain)
    grad_inputs = (grad_first + grad_tokens).astype(BF)[None]

    late_cols = query_cols + lat_cols // 4
    late = jnp.concatenate(
        [
            grad_wq.astype(BF),
            grad_wl.astype(BF),
            grad_attn[:, None].astype(BF),
            jnp.zeros((width, -(late_cols + 1) % LANES), BF),
        ],
        axis=1,
    )
    late = finish(late.reshape(nz, 2, local_rows, -1), nz, 13).reshape(4, local_rows, -1)
    grad_wq = jnp.concatenate(
        [
            late[:, :, :nope_cols].reshape(4, local_rows, heads, NOPE),
            late[:, :, nope_cols : nope_cols + rope_cols].reshape(4, local_rows, heads, -1),
            late[:, :, nope_cols + rope_cols : query_cols].reshape(4, local_rows, heads, -1),
        ],
        axis=3,
    )
    grad_wq = columns_of(grad_wq.reshape(4, local_rows, -1)).astype(F32)
    grad_wl = columns_of(late[:, :, query_cols:late_cols]).astype(F32)
    grad_attn = jnp.sum(late[:, :, late_cols].astype(F32), axis=0)
    return (
        output,
        grad_inputs,
        grad_attn,
        grad_wq,
        grad_wl,
        grad_lat_gain,
        grad_we,
        grad_wo,
        grad_ffn,
        grad_wr,
        shared_in,
        shared_out,
        grad_in,
        grad_down,
    )


def rotate(operand, cosine, sine_part):
    half_width = operand.shape[-1] // 2
    former = operand[..., :half_width]
    latter = operand[..., half_width:]
    return jnp.concatenate(
        [former * cosine - latter * sine_part, latter * cosine + former * sine_part], axis=-1
    )


def across(left_side, right_side):
    return lax.dot_general(
        left_side, right_side, (((0,), (0,)), ((), ())), preferred_element_type=jnp.float32
    )


def against(left_side, right_side):
    return lax.dot_general(
        left_side, right_side, (((1,), (1,)), ((), ())), preferred_element_type=jnp.float32
    )


def to_experts(buffer):
    return lax.all_to_all(buffer, "expert", split_axis=0, concat_axis=2, tiled=True)


def from_experts(buffer):
    return lax.all_to_all(buffer, "expert", split_axis=2, concat_axis=0, tiled=True)


def share_rows(row_block):
    return lax.all_gather(row_block, ("dp", "ctx"), axis=1, tiled=True)


def sum_rows(partial_value):
    return lax.psum_scatter(
        partial_value.astype(jnp.bfloat16), ("dp", "ctx"), scatter_dimension=1, tiled=True
    ).astype(jnp.float32)


def key_scores(query_r, keys_nope, keys_rope, allowed, scale_factor):
    scores = jnp.einsum(
        "qhd,khd->hqk", query_r[..., :NOPE], keys_nope, preferred_element_type=jnp.float32
    )
    scores = scores + jnp.einsum(
        "qhd,kd->hqk", query_r[..., NOPE:], keys_rope, preferred_element_type=jnp.float32
    )
    return jnp.where(allowed[None], scores * scale_factor, -1e30)


def general_body(
    layer_input,
    cotangent,
    routes,
    attn_gain,
    w_query,
    w_latent,
    latent_gain,
    w_expand,
    w_output,
    ffn_gain,
    w_router,
    w_shared_in,
    w_shared_out,
    w_expert_in,
    w_expert_out,
):
    (
        weight_query,
        weight_latent,
        weight_expand,
        weight_output,
        weight_router,
        weight_shared_in,
        weight_shared_out,
    ) = (
        lax.all_gather(w_query, "expert", axis=0, tiled=True),
        lax.all_gather(w_latent, "expert", axis=0, tiled=True),
        lax.all_gather(w_expand, "expert", axis=0, tiled=True),
        lax.all_gather(w_output, "expert", axis=0, tiled=True),
        lax.all_gather(w_router, "expert", axis=0, tiled=True),
        lax.all_gather(w_shared_in, "expert", axis=0, tiled=True),
        lax.all_gather(w_shared_out, "expert", axis=0, tiled=True),
    )
    tokens = layer_input[0].astype(jnp.float32)
    tok_count = tokens.shape[0]
    row_width = tokens.shape[1]
    experts = weight_router.shape[1]
    groups = lax.axis_size("expert")
    local_experts = experts // groups
    capacity = tok_count * TOP * 4 // (3 * experts)
    assigns = tok_count * TOP
    shared_width = weight_shared_out.shape[0]
    places = lax.axis_index("ctx") * tok_count + jnp.arange(tok_count, dtype=jnp.int32)
    inverse = 10000.0 ** (-jnp.arange(0, ROPE, 2).astype(jnp.float32) / ROPE)
    angles = places.astype(jnp.float32)[:, None] * inverse[None, :]
    cosine = jnp.cos(angles)
    sine_part = jnp.sin(angles)
    normed_one, factor_one = normalize(tokens)
    hidden_one = (normed_one * attn_gain).astype(jnp.bfloat16)
    queries = jnp.dot(hidden_one, weight_query, preferred_element_type=jnp.float32).reshape(
        tok_count, HEADS, NOPE + ROPE
    )
    query_r = jnp.concatenate(
        [
            queries[..., :NOPE],
            rotate(queries[..., NOPE:], cosine[:, None, :], sine_part[:, None, :]),
        ],
        axis=-1,
    ).astype(jnp.bfloat16)
    latent = jnp.dot(hidden_one, weight_latent, preferred_element_type=jnp.float32)
    normed_lat, factor_lat = normalize(latent[:, :KV])
    compressed = (normed_lat * latent_gain).astype(jnp.bfloat16)
    key_rope = rotate(latent[:, KV:], cosine, sine_part).astype(jnp.bfloat16)
    packed = jnp.concatenate([compressed, key_rope], axis=1)
    all_keys = lax.all_gather(packed, "ctx", axis=0, tiled=True)
    every_comp = all_keys[:, :KV]
    every_rope = all_keys[:, KV:]
    expanded = (
        jnp.dot(every_comp, weight_expand, preferred_element_type=jnp.float32)
        .astype(jnp.bfloat16)
        .reshape(-1, HEADS, NOPE + VH)
    )
    keys_nope = expanded[..., :NOPE]
    values = expanded[..., NOPE:]
    scale_factor = 1.0 / math.sqrt(NOPE + ROPE)
    allowed = jnp.arange(all_keys.shape[0], dtype=jnp.int32)[None, :] <= places[:, None]
    scores = key_scores(query_r, keys_nope, every_rope, allowed, scale_factor)
    highest = jnp.max(scores, axis=-1, keepdims=True)
    exponent = jnp.exp(scores - highest)
    totals = jnp.sum(exponent, axis=-1, keepdims=True)
    logsum = highest + jnp.log(totals)
    weights = (exponent / totals).astype(jnp.bfloat16)
    mixed_heads = (
        jnp.einsum("hqk,khd->qhd", weights, values, preferred_element_type=jnp.float32)
        .reshape(tok_count, HEADS * VH)
        .astype(jnp.bfloat16)
    )
    first_sum = tokens + jnp.dot(mixed_heads, weight_output, preferred_element_type=jnp.float32)
    normed_two, factor_two = normalize(first_sum)
    hidden_two = (normed_two * ffn_gain).astype(jnp.bfloat16)
    logits = jnp.dot(hidden_two, weight_router, preferred_element_type=jnp.float32)
    router_top = jnp.max(logits, axis=-1, keepdims=True)
    router_exp = jnp.exp(logits - router_top)
    router = router_exp / jnp.sum(router_exp, axis=-1, keepdims=True)
    own_routes = routes[0]
    chosen = own_routes[:, :, None] == jnp.arange(experts, dtype=jnp.int32)[None, None, :]
    picked = jnp.sum(jnp.where(chosen, router[:, None, :], 0.0), axis=2)
    shared_gu = jnp.dot(hidden_two, weight_shared_in, preferred_element_type=jnp.float32)
    shared_gate = shared_gu[:, :shared_width]
    shared_up = shared_gu[:, shared_width:]
    shared_silu, shared_slope = silu_parts(shared_gate)
    shared_act = (shared_silu * shared_up).astype(jnp.bfloat16)
    shared = jnp.dot(shared_act, weight_shared_out, preferred_element_type=jnp.float32)
    picked_ids = own_routes.reshape(-1)
    onehot = (picked_ids[:, None] == jnp.arange(experts, dtype=jnp.int32)[None, :]).astype(
        jnp.int32
    )
    position = jnp.sum((jnp.cumsum(onehot, axis=0) - onehot) * onehot, axis=1)
    target = picked_ids * capacity + position
    holder = (
        jnp.full((experts * capacity,), assigns, jnp.int32)
        .at[target]
        .set(jnp.arange(assigns, dtype=jnp.int32))
    )
    padded = jnp.concatenate([hidden_two, jnp.zeros((1, row_width), jnp.bfloat16)], axis=0)
    outgoing = padded[holder // TOP].reshape(groups, local_experts, capacity, row_width)
    incoming = to_experts(outgoing)[0]
    expert_input = share_rows(incoming)
    paired = jnp.einsum(
        "erd,egfd->ergf", expert_input, w_expert_in, preferred_element_type=jnp.float32
    )
    expert_gate = paired[:, :, 0]
    expert_up = paired[:, :, 1]
    expert_silu, expert_slope = silu_parts(expert_gate)
    expert_act = (expert_silu * expert_up).astype(jnp.bfloat16)
    partial_value = jnp.einsum(
        "erf,efd->erd", expert_act, w_expert_out, preferred_element_type=jnp.float32
    )
    expert_out = sum_rows(partial_value).astype(jnp.bfloat16)
    returned = from_experts(expert_out[None]).reshape(experts * capacity, row_width)
    gathered = returned[target].reshape(tok_count, TOP, row_width).astype(jnp.float32)
    routed = jnp.sum(picked[:, :, None] * gathered, axis=1)
    output = (first_sum + shared + routed).astype(jnp.bfloat16)[None]
    grad_out = cotangent[0].astype(jnp.float32)
    grad_picked = jnp.sum(grad_out[:, None, :] * gathered, axis=2)
    sending = (
        (picked[:, :, None] * grad_out[:, None, :]).astype(jnp.bfloat16).reshape(assigns, row_width)
    )
    sending = jnp.concatenate([sending, jnp.zeros((1, row_width), jnp.bfloat16)], axis=0)[holder]
    grad_expert_out = to_experts(sending.reshape(groups, local_experts, capacity, row_width))[0]
    grad_expert_out = share_rows(grad_expert_out)
    grad_act = jnp.einsum(
        "erd,efd->erf", grad_expert_out, w_expert_out, preferred_element_type=jnp.float32
    )
    grad_weight_out = jnp.einsum(
        "erf,erd->efd", expert_act, grad_expert_out, preferred_element_type=jnp.float32
    )
    grad_paired = jnp.stack(
        [grad_act * expert_up * expert_slope, grad_act * expert_silu], axis=2
    ).astype(jnp.bfloat16)
    grad_weight_in = jnp.einsum(
        "ergf,erd->egfd", grad_paired, expert_input, preferred_element_type=jnp.float32
    )
    grad_input_part = jnp.einsum(
        "ergf,egfd->erd", grad_paired, w_expert_in, preferred_element_type=jnp.float32
    )
    grad_rows_sum = sum_rows(grad_input_part)
    grad_back = from_experts(grad_rows_sum.astype(jnp.bfloat16)[None]).reshape(
        experts * capacity, row_width
    )
    grad_hidden_two = jnp.sum(
        grad_back[target].reshape(tok_count, TOP, row_width).astype(jnp.float32), axis=1
    )
    grad_router = jnp.sum(jnp.where(chosen, grad_picked[:, :, None], 0.0), axis=1)
    grad_logits = (
        router * (grad_router - jnp.sum(router * grad_router, axis=1, keepdims=True))
    ).astype(jnp.bfloat16)
    grad_router_weight = across(hidden_two, grad_logits)
    grad_hidden_two = grad_hidden_two + against(grad_logits, weight_router)
    grad_low = grad_out.astype(jnp.bfloat16)
    grad_shared_out = across(shared_act, grad_low)
    grad_shared_act = against(grad_low, weight_shared_out)
    grad_shared_gu = jnp.concatenate(
        [grad_shared_act * shared_up * shared_slope, grad_shared_act * shared_silu], axis=1
    ).astype(jnp.bfloat16)
    grad_shared_in = across(hidden_two, grad_shared_gu)
    grad_hidden_two = grad_hidden_two + against(grad_shared_gu, weight_shared_in)
    grad_first_norm, grad_ffn = norm_back(grad_hidden_two, normed_two, factor_two, ffn_gain)
    grad_first = grad_out + grad_first_norm
    grad_first_low = grad_first.astype(jnp.bfloat16)
    grad_output_weight = across(mixed_heads, grad_first_low)
    grad_mixed = (
        against(grad_first_low, weight_output).astype(jnp.bfloat16).reshape(tok_count, HEADS, VH)
    )
    prob_rows = jnp.exp(key_scores(query_r, keys_nope, every_rope, allowed, scale_factor) - logsum)
    grad_weights = jnp.einsum(
        "qhd,khd->hqk", grad_mixed, values, preferred_element_type=jnp.float32
    )
    grad_scores = (
        prob_rows * (grad_weights - jnp.sum(prob_rows * grad_weights, axis=-1, keepdims=True))
    ).astype(jnp.bfloat16)
    grad_query_nope = (
        jnp.einsum("hqk,khd->qhd", grad_scores, keys_nope, preferred_element_type=jnp.float32)
        * scale_factor
    )
    grad_query_rope = (
        jnp.einsum("hqk,kd->qhd", grad_scores, every_rope, preferred_element_type=jnp.float32)
        * scale_factor
    )
    grad_keys_nope = (
        jnp.einsum(
            "hqk,qhd->khd", grad_scores, query_r[..., :NOPE], preferred_element_type=jnp.float32
        )
        * scale_factor
    )
    grad_keys_rope = (
        jnp.einsum(
            "hqk,qhd->kd", grad_scores, query_r[..., NOPE:], preferred_element_type=jnp.float32
        )
        * scale_factor
    )
    grad_values = jnp.einsum(
        "hqk,qhd->khd", weights, grad_mixed, preferred_element_type=jnp.float32
    )
    grad_expanded = (
        jnp.concatenate([grad_keys_nope, grad_values], axis=-1)
        .reshape(all_keys.shape[0], -1)
        .astype(jnp.bfloat16)
    )
    grad_expand_weight = across(every_comp, grad_expanded)
    grad_every_comp = against(grad_expanded, weight_expand)
    grad_comp, grad_rope_key = (
        lax.psum_scatter(
            grad_every_comp.astype(jnp.bfloat16), "ctx", scatter_dimension=0, tiled=True
        ).astype(jnp.float32),
        lax.psum_scatter(
            grad_keys_rope.astype(jnp.bfloat16), "ctx", scatter_dimension=0, tiled=True
        ).astype(jnp.float32),
    )
    grad_lat_comp, grad_lat_gain = norm_back(grad_comp, normed_lat, factor_lat, latent_gain)
    grad_latent = jnp.concatenate(
        [grad_lat_comp, rotate(grad_rope_key, cosine, -sine_part)], axis=1
    ).astype(jnp.bfloat16)
    grad_query = (
        jnp.concatenate(
            [grad_query_nope, rotate(grad_query_rope, cosine[:, None, :], -sine_part[:, None, :])],
            axis=-1,
        )
        .reshape(tok_count, -1)
        .astype(jnp.bfloat16)
    )
    grad_query_weight = across(hidden_one, grad_query)
    grad_latent_weight = across(hidden_one, grad_latent)
    grad_hidden_one = against(grad_query, weight_query) + against(grad_latent, weight_latent)
    grad_tokens, grad_attn = norm_back(grad_hidden_one, normed_one, factor_one, attn_gain)
    grad_inputs = (grad_first + grad_tokens).astype(jnp.bfloat16)[None]
    sliced = (
        lax.psum_scatter(
            grad_query_weight.astype(jnp.bfloat16), "expert", scatter_dimension=0, tiled=True
        ).astype(jnp.float32),
        lax.psum_scatter(
            grad_latent_weight.astype(jnp.bfloat16), "expert", scatter_dimension=0, tiled=True
        ).astype(jnp.float32),
        lax.psum_scatter(
            grad_expand_weight.astype(jnp.bfloat16), "expert", scatter_dimension=0, tiled=True
        ).astype(jnp.float32),
        lax.psum_scatter(
            grad_output_weight.astype(jnp.bfloat16), "expert", scatter_dimension=0, tiled=True
        ).astype(jnp.float32),
        lax.psum_scatter(
            grad_router_weight.astype(jnp.bfloat16), "expert", scatter_dimension=0, tiled=True
        ).astype(jnp.float32),
        lax.psum_scatter(
            grad_shared_in.astype(jnp.bfloat16), "expert", scatter_dimension=0, tiled=True
        ).astype(jnp.float32),
        lax.psum_scatter(
            grad_shared_out.astype(jnp.bfloat16), "expert", scatter_dimension=0, tiled=True
        ).astype(jnp.float32),
        lax.psum_scatter(
            grad_attn.astype(jnp.bfloat16), "expert", scatter_dimension=0, tiled=True
        ).astype(jnp.float32),
        lax.psum_scatter(
            grad_lat_gain.astype(jnp.bfloat16), "expert", scatter_dimension=0, tiled=True
        ).astype(jnp.float32),
        lax.psum_scatter(
            grad_ffn.astype(jnp.bfloat16), "expert", scatter_dimension=0, tiled=True
        ).astype(jnp.float32),
    )
    summed = (
        lax.psum(sliced[0].astype(jnp.bfloat16), ("dp", "ctx")).astype(jnp.float32),
        lax.psum(sliced[1].astype(jnp.bfloat16), ("dp", "ctx")).astype(jnp.float32),
        lax.psum(sliced[2].astype(jnp.bfloat16), ("dp", "ctx")).astype(jnp.float32),
        lax.psum(sliced[3].astype(jnp.bfloat16), ("dp", "ctx")).astype(jnp.float32),
        lax.psum(sliced[4].astype(jnp.bfloat16), ("dp", "ctx")).astype(jnp.float32),
        lax.psum(sliced[5].astype(jnp.bfloat16), ("dp", "ctx")).astype(jnp.float32),
        lax.psum(sliced[6].astype(jnp.bfloat16), ("dp", "ctx")).astype(jnp.float32),
        lax.psum(sliced[7].astype(jnp.bfloat16), ("dp", "ctx")).astype(jnp.float32),
        lax.psum(sliced[8].astype(jnp.bfloat16), ("dp", "ctx")).astype(jnp.float32),
        lax.psum(sliced[9].astype(jnp.bfloat16), ("dp", "ctx")).astype(jnp.float32),
    )
    return (
        output,
        grad_inputs,
        summed[7],
        summed[0],
        summed[1],
        summed[8],
        summed[2],
        summed[3],
        summed[9],
        summed[4],
        summed[5],
        summed[6],
        grad_weight_in,
        grad_weight_out,
    )


def solution(mesh):
    dense = mesh.shape["dp"] == 2 and mesh.shape["ctx"] == 2 and mesh.shape["expert"] == 8
    return jax.shard_map(
        split_body if dense else general_body,
        mesh=mesh,
        in_specs=(
            P(("dp", "expert"), "ctx", None),
            P(("dp", "expert"), "ctx", None),
            P(("dp", "expert"), "ctx", None),
            P(),
            P("expert", None),
            P("expert", None),
            P(),
            P("expert", None),
            P("expert", None),
            P(),
            P("expert", None),
            P("expert", None),
            P("expert", None),
            P("expert", None, ("dp", "ctx"), None),
            P("expert", ("dp", "ctx"), None),
        ),
        out_specs=(
            P(("dp", "expert"), "ctx", None),
            P(("dp", "expert"), "ctx", None),
            P("expert"),
            P("expert", None),
            P("expert", None),
            P("expert"),
            P("expert", None),
            P("expert", None),
            P("expert"),
            P("expert", None),
            P("expert", None),
            P("expert", None),
            P("expert", None, ("dp", "ctx"), None),
            P("expert", ("dp", "ctx"), None),
        ),
        check_vma=False,
    )
```
